32 devices in a mesh: row: 4 (over z), col: 2 (over x), dp: 4 (over y, core).
Axes of the slice: x: 2, y: 2, z: 4, core: 2. Of those that a mesh axis runs over, the one named last changes fastest.
Arguments:
- tokens: bfloat16 [1536, 6144], P('dp', 'row'), parts along dimension 0, may hold values from -120 to 120
- norm_gain: float32 [6144], P('row'), may hold values from 0.25 to 1.75
- qkv_weight: bfloat16 [6144, 3, 3072], P('row', None, 'col'), may hold values from -2.5 to 2.5
- out_weight: bfloat16 [3072, 6144], P('col', 'row'), may hold values from -0.109375 to 0.109375
Outputs:
- projected: bfloat16 [1536, 6144], P('dp', 'row'), parts along dimension 0
The draws below stay inside these ranges and needn't reach their ends.
There are 4 independent parts, one for each index of `dp`. The reference program is written for one: setup_inputs(seed, part) draws one part's arguments, and reference() takes and returns one part's arrays. A program takes and returns all parts, laid end to end along the dimension named above; an argument that names none is the same for every part. Nothing has to cross between parts.
All inputs are finite; a program needn't handle non-finite values.
Results may differ from the reference program's by a relative error of at most 0.025.
Values may be sent and summed in bfloat16 or wider, within the bound.
A program may use at most 64 MiB of HBM per device.

```python
import math
import jax
import jax.numpy as jnp
from jax import lax

D = 6144
H = 24
K = 128
SEQ = 384
N_ROW = 4


def draw_tokens(key, part):
    subkeys = jax.random.split(key, 4)
    position = jnp.arange(D, dtype=jnp.float32) / D
    texture = jnp.exp(jax.random.uniform(subkeys[0], (1, D), jnp.float32, jnp.log(0.7), jnp.log(1.4)))
    row_scale = jnp.exp(jax.random.uniform(subkeys[1], (SEQ, 1), jnp.float32, jnp.log(0.5), jnp.log(2.0)))
    offset = jnp.clip(jax.random.normal(subkeys[2], (SEQ, 1), jnp.float32), -3.0, 3.0)
    feature_ramp = 10.0 ** (position - 0.5)
    jitter = jnp.clip(jax.random.normal(subkeys[3], (SEQ, D), jnp.float32), -4.0, 4.0)
    values = row_scale * feature_ramp * (offset + jitter * texture)
    return jnp.clip(values, -120.0, 120.0).astype(jnp.bfloat16)


def draw_qkv_weight(key, part):
    subkeys = jax.random.split(key, 1)
    weights = jnp.clip(jax.random.normal(subkeys[0], (D, 3, H * K), jnp.float32), -6.0, 6.0) / math.sqrt(D)
    return jnp.clip(weights, -2.5, 2.5).astype(jnp.bfloat16)


def block_scale(own_key, dims, cuts, low, top_value):
    level = 1.0
    for axis_at, blocks in cuts:
        heights = jax.random.uniform(jax.random.fold_in(jax.random.fold_in(own_key, 6), axis_at), (blocks,), jnp.float32, low / len(cuts), top_value / len(cuts))
        level = level * jnp.repeat(jnp.exp(heights), dims[axis_at] // blocks).reshape((-1,) + (1,) * (len(dims) - 1 - axis_at))
    return level


def bell_draw(stream_key, dims, deviation, reach, shards=(), kind=jnp.bfloat16):
    level = block_scale(stream_key, dims, shards, -0.22, 0.18) if shards else 1.0
    entries = jax.random.normal(stream_key, dims, jnp.float32) * deviation * level
    return jnp.minimum(jnp.maximum(entries, -reach), reach).astype(kind)


def setup_inputs(seed: int = 0, part: int = 0) -> dict:
    key_of = jax.random.split(jax.random.key(seed), 5)
    part_splits = jax.random.split(jax.random.fold_in(key_of[4], part), 5)
    return {
        "tokens": draw_tokens(jax.random.fold_in(jax.random.fold_in(key_of[4], part), 71), part),
        "norm_gain": jnp.clip(1.0 + 0.15 * jax.random.normal(key_of[1], (D,), jnp.float32), 0.25, 1.75),
        "qkv_weight": draw_qkv_weight(jax.random.fold_in(key_of[4], 71), part),
        "out_weight": bell_draw(key_of[3], (H * K, D), (H * K) ** -0.5, 0.109375, ((0, 2), (1, 4))),
    }


EPSILON = 1e-05

def normalize(tokens, norm_gain):
    values = tokens.astype(jnp.float32)
    average = lax.optimization_barrier(jnp.mean(values, axis=1, keepdims=True))
    centered = values - average
    variance = lax.optimization_barrier(jnp.mean(centered * centered, axis=1, keepdims=True))
    return (centered * lax.rsqrt(variance + EPSILON) * norm_gain).astype(jnp.bfloat16)

def project(normed, qkv_weight):
    block_width = D // N_ROW
    flattened = qkv_weight.reshape(D, 3 * H * K)
    totals = jnp.zeros((SEQ, 3 * H * K), jnp.float32)
    for row_block in range(N_ROW):
        first_feature = row_block * block_width
        partial_value = jnp.dot(normed[:, first_feature:first_feature + block_width], flattened[first_feature:first_feature + block_width], preferred_element_type=jnp.float32)
        rounded = lax.optimization_barrier(partial_value.astype(jnp.bfloat16))
        totals = totals + rounded.astype(jnp.float32)
    return totals.astype(jnp.bfloat16).reshape(SEQ, 3, H, K)

def attend_head(operands):
    query_part, key_part, value_part = operands
    scores = jnp.dot(query_part, key_part.T, preferred_element_type=jnp.float32) * (1.0 / math.sqrt(K))
    largest = lax.optimization_barrier(jnp.max(scores, axis=1, keepdims=True))
    exponent = jnp.exp(scores - largest)
    softmax_weights = (exponent / lax.optimization_barrier(jnp.sum(exponent, axis=1, keepdims=True))).astype(jnp.bfloat16)
    return jnp.dot(softmax_weights, value_part, preferred_element_type=jnp.float32).astype(jnp.bfloat16)

def reference(tokens, norm_gain, qkv_weight, out_weight):
    normed = normalize(tokens, norm_gain)
    stacked = jnp.transpose(project(normed, qkv_weight), (1, 2, 0, 3))
    attended = lax.map(attend_head, (stacked[0], stacked[1], stacked[2]))
    attended = jnp.transpose(attended, (1, 0, 2)).reshape(SEQ, H * K)
    return jnp.dot(attended, out_weight, preferred_element_type=jnp.float32).astype(jnp.bfloat16)
```

```python
import functools
import math

import jax
import jax.numpy as jnp
from jax import lax
from jax.experimental import pallas as pl
from jax.experimental.pallas import tpu as pltpu
from jax.sharding import PartitionSpec as P

K = 128


EPSILON = 1e-05


def attend(queries, key_rows, value_rows):
    query_total = queries.shape[0]
    head_count = queries.shape[1] // K
    scaling = 1.0 / math.sqrt(K)
    split_keys = key_rows.reshape(key_rows.shape[0], head_count, K)
    split_values = value_rows.reshape(value_rows.shape[0], head_count, K)
    split_queries = queries.reshape(query_total, head_count, K)
    scores = (
        jnp.einsum("qhd,khd->hqk", split_queries, split_keys, preferred_element_type=jnp.float32)
        * scaling
    )
    largest = jnp.max(scores, axis=2, keepdims=True)
    exponent = jnp.exp(scores - largest)
    softmax_weights = (exponent / jnp.sum(exponent, axis=2, keepdims=True)).astype(jnp.bfloat16)
    mixed = jnp.einsum(
        "hqk,khd->qhd", softmax_weights, split_values, preferred_element_type=jnp.float32
    )
    result = mixed.astype(jnp.bfloat16)
    return result.reshape(query_total, head_count * K)


def shards(tokens, norm_gain, qkv_weight, out_weight):
    row_count, block_width = tokens.shape
    full_width = block_width * lax.axis_size("row")
    values = tokens.astype(jnp.float32)
    totals, squares = lax.psum(
        (jnp.sum(values, axis=1, keepdims=True), jnp.sum(values * values, axis=1, keepdims=True)),
        "row",
    )
    average = totals / full_width
    variance = squares / full_width - average * average
    centered = values - average
    normed = (centered * lax.rsqrt(variance + EPSILON) * norm_gain).astype(jnp.bfloat16)
    head_columns = qkv_weight.shape[2]
    partial_value = jnp.dot(
        normed,
        qkv_weight.reshape(block_width, 3 * head_columns),
        preferred_element_type=jnp.float32,
    )
    summed = lax.psum(partial_value.astype(jnp.bfloat16), "row").reshape(row_count, 3, head_columns)
    attended = attend(summed[:, 0], summed[:, 1], summed[:, 2])
    partial_out = jnp.dot(attended, out_weight, preferred_element_type=jnp.float32)
    return lax.psum(partial_out.astype(jnp.bfloat16), "col")


MESH = pl.DeviceIdType.MESH
WIDE = 2 * K
ROWS = 32
PIECE = 128


def sublayer_kernel(
    rows_n, dp_n, tok_hbm, gain_ref, w_hbm, wo_hbm, out_hbm,
    tok, wide_w, gain_row, stat_col, stats, normed, arrived, summed, attended, late_w, total, out,
    tok_sem, w_sem, late_sem, out_sem, st_send, st_recv, rs_send, rs_recv, at_send, at_recv,
    la_send, la_recv, lx_send, lx_recv, ly_send, ly_recv, lc_send, lc_recv, ld_send, ld_recv,
):
    z = lax.axis_index("row")
    col = lax.axis_index("col")
    dp = lax.axis_index("dp")
    tokens_n, block = tok.shape
    half = w_hbm.shape[2] // 2
    pairs = half // WIDE
    chunks = 3 * pairs
    tiles = block // WIDE
    pieces = tokens_n // PIECE
    quarter = WIDE // dp_n
    partner = {"col": 1 - col}
    sibling_at = dp + 1 - 2 * (dp % 2)
    across_at = (dp + 2) % dp_n
    sibling, across = {"dp": sibling_at}, {"dp": across_at}
    scaling = 1.0 / math.sqrt(K)
    last_place = rows_n - 1

    def weight_copy(d, c):
        pair, kind = c // 3, (c + 1) % 3
        first = pl.multiple_of(d * half + pair * WIDE, WIDE)
        return pltpu.make_async_copy(
            w_hbm.at[kind, :, pl.ds(first, WIDE)], wide_w.at[d, c], w_sem.at[d, c]
        )

    tok_copy = pltpu.make_async_copy(tok_hbm, tok, tok_sem)
    tok_copy.start()

    @pl.loop(0, chunks)
    def _(c):
        weight_copy(0, c).start()
        weight_copy(1, c).start()

    def own_copy(d, p):
        rows = pl.ds(d * half + p * WIDE, WIDE)
        return pltpu.make_async_copy(wo_hbm.at[rows], late_w.at[col, d, p], late_sem.at[d, p])

    def quarter_at(which):
        return pl.ds(pl.multiple_of(which * quarter, quarter), quarter)

    def share_copy(d, p, owner):
        first = pl.multiple_of(d * half + p * WIDE + dp * quarter, quarter)
        return pltpu.make_async_remote_copy(
            src_ref=wo_hbm.at[pl.ds(first, quarter)],
            dst_ref=late_w.at[owner, d, p, quarter_at(dp)],
            send_sem=lx_send.at[d, p], recv_sem=lx_recv.at[d, p], device_id=partner,
            device_id_type=MESH,
        )

    def pass_copy(d, p, which, sends, recvs, device):
        piece = late_w.at[1 - col, d, p, quarter_at(which)]
        return pltpu.make_async_remote_copy(
            src_ref=piece, dst_ref=piece, send_sem=sends.at[d, p], recv_sem=recvs.at[d, p],
            device_id=device, device_id_type=MESH,
        )

    def across_copy(d, p, which):
        return pass_copy(d, p, which, ly_send, ly_recv, across)

    def near_copy(d, p, which):
        return pass_copy(d, p, which, lc_send, lc_recv, sibling)

    def far_copy(d, p, which):
        return pass_copy(d, p, which, ld_send, ld_recv, sibling)

    blocks = [(d, p) for p in range(pairs) for d in range(2)]
    for d, p in blocks:
        own_copy(d, p).start()

    barrier = pltpu.get_barrier_semaphore()
    for o in range(1, rows_n):
        pl.semaphore_signal(
            barrier, inc=1, device_id={"row": lax.rem(z + o, rows_n)}, device_id_type=MESH
        )
    for device in (partner, sibling, across):
        pl.semaphore_signal(barrier, inc=1, device_id=device, device_id_type=MESH)

    for j in range(block // 128):
        gain_row[0:1, j * 128:(j + 1) * 128] = gain_ref[j:j + 1, :]
    tok_copy.wait()

    @pl.loop(0, tokens_n // ROWS)
    def _(i):
        at = pl.ds(pl.multiple_of(i * ROWS, ROWS), ROWS)
        x = tok[at, :].astype(jnp.float32)
        mean = jnp.sum(x, axis=1, keepdims=True) * (1.0 / block)
        away = x - mean
        square = jnp.sum(away * away, axis=1, keepdims=True)
        stat_col[0, at, :] = jnp.broadcast_to(mean, (ROWS, 128))
        stat_col[1, at, :] = jnp.broadcast_to(square, (ROWS, 128))

    stats[z, 0] = stat_col[0].T[0:8]
    stats[z, 1] = stat_col[1].T[0:8]
    pl.semaphore_wait(barrier, rows_n + 2)

    def stat_copy(o):
        return pltpu.make_async_remote_copy(
            src_ref=stats.at[z], dst_ref=stats.at[z], send_sem=st_send.at[o],
            recv_sem=st_recv.at[z], device_id={"row": lax.rem(z + o, rows_n)},
            device_id_type=MESH,
        )

    def stat_arrival(o):
        source = lax.rem(z + o, rows_n)
        return pltpu.make_async_remote_copy(
            src_ref=stats.at[source], dst_ref=stats.at[source], send_sem=st_send.at[o],
            recv_sem=st_recv.at[source], device_id={"row": source}, device_id_type=MESH,
        )

    for o in range(1, rows_n):
        stat_copy(o).start()
    for d, p in blocks:
        share_copy(d, p, col).start()
    for o in range(1, rows_n):
        stat_arrival(o).wait_recv()
    mean = sum(stats[i, 0] for i in range(rows_n)) * (1.0 / rows_n)
    spread = sum(
        stats[i, 1] * (1.0 / block) + (stats[i, 0] - mean) * (stats[i, 0] - mean)
        for i in range(rows_n)
    ) * (1.0 / rows_n)
    scale = lax.rsqrt(spread + EPSILON)
    stat_col[0] = jnp.broadcast_to(mean[0:1], (128, tokens_n)).T
    stat_col[1] = jnp.broadcast_to(scale[0:1], (128, tokens_n)).T

    @pl.loop(0, tokens_n // ROWS)
    def _(i):
        at = pl.ds(pl.multiple_of(i * ROWS, ROWS), ROWS)
        x = tok[at, :].astype(jnp.float32)
        away = (x - stat_col[0, at, 0:1]) * stat_col[1, at, 0:1]
        normed[at, :] = (away * gain_row[...]).astype(jnp.bfloat16)

    def place(d):
        return z if d == 1 else last_place - z

    def onward(d):
        return {"row": jnp.clip(z + 1 if d == 1 else z - 1, 0, last_place)}

    def back(d):
        return {"row": jnp.clip(z - 1 if d == 1 else z + 1, 0, last_place)}

    def sum_copy(d, c, i):
        at = pl.ds(i * PIECE, PIECE)
        return pltpu.make_async_remote_copy(
            src_ref=summed.at[d, c, at], dst_ref=arrived.at[d, c, at],
            send_sem=rs_send.at[d, c, i], recv_sem=rs_recv.at[d, c, i],
            device_id=onward(d), device_id_type=MESH,
        )

    def attended_copy(d, p, i):
        piece = attended.at[col, d, p, pl.ds(i * PIECE, PIECE)]
        return pltpu.make_async_remote_copy(
            src_ref=piece, dst_ref=piece, send_sem=at_send.at[d, p, i],
            recv_sem=at_recv.at[d, p, i], device_id=back(d), device_id_type=MESH,
        )

    def cross_copy(d, p, i, owner):
        piece = attended.at[owner, d, p, pl.ds(i * PIECE, PIECE)]
        return pltpu.make_async_remote_copy(
            src_ref=piece, dst_ref=piece, send_sem=la_send.at[d, p, i],
            recv_sem=la_recv.at[d, p, i], device_id=partner, device_id_type=MESH,
        )

    def attend_piece(d, p, i):
        rows = pl.ds(i * PIECE, PIECE)
        for h in range(2):
            at = slice(h * K, (h + 1) * K)
            k = summed[d, 3 * p, :, at]
            v = summed[d, 3 * p + 1, :, at]
            q = summed[d, 3 * p + 2, rows, at]
            scores = lax.dot_general(
                q, k, (((1,), (1,)), ((), ())), preferred_element_type=jnp.float32
            ) * scaling
            exponent = jnp.exp(scores - jnp.max(scores, axis=1, keepdims=True))
            weights = exponent / jnp.sum(exponent, axis=1, keepdims=True)
            attended[col, d, p, rows, at] = jnp.dot(
                weights.astype(jnp.bfloat16), v, preferred_element_type=jnp.float32
            ).astype(jnp.bfloat16)

    def weights_ready(p):
        for d in range(2):
            own_copy(d, p).wait()
            near_copy(d, p, sibling_at).wait_recv()
            far_copy(d, p, (sibling_at + 2) % dp_n).wait_recv()

    def fold(p, rows, at):
        return sum(
            jnp.dot(
                attended[owner, d, p, rows], late_w[owner, d, p, :, at],
                preferred_element_type=jnp.float32,
            )
            for owner in range(2) for d in range(2)
        )

    slots = chunks + 2 * last_place
    every = pl.ds(0, tokens_n)

    @pl.loop(0, slots)
    def _(t):
        for d in range(2):
            pos = place(d)
            c = t - pos

            @pl.when((c >= 0) & (c < chunks))
            def _():
                weight_copy(d, c).wait()
                part = jnp.dot(normed[...], wide_w[d, c], preferred_element_type=jnp.float32)

                for i in range(pieces):
                    at = pl.ds(i * PIECE, PIECE)
                    share = part[i * PIECE:(i + 1) * PIECE]

                    @pl.when(pos == 0)
                    def _():
                        summed[d, c, at] = share.astype(jnp.bfloat16)

                    @pl.when(pos > 0)
                    def _():
                        sum_copy(d, c, i).wait_recv()
                        whole = share + arrived[d, c, at].astype(jnp.float32)
                        summed[d, c, at] = whole.astype(jnp.bfloat16)

                    @pl.when(pos < last_place)
                    def _():
                        sum_copy(d, c, i).start()

                    @pl.when((pos == last_place) & (c % 3 == 2))
                    def _():
                        attend_piece(d, c // 3, i)
                        attended_copy(d, c // 3, i).start()
                        cross_copy(d, c // 3, i, col).start()

        for d in range(2):
            pos = place(d)
            e = t - last_place - (last_place - pos)
            p = e // 3

            @pl.when((pos < last_place) & (e >= 0) & (e < chunks) & (e % 3 == 2))
            def _():
                for i in range(pieces):
                    attended_copy(d, p, i).wait_recv()

                    @pl.when(pos > 0)
                    def _():
                        attended_copy(d, p, i).start()

                    cross_copy(d, p, i, col).start()

        for b, (d, p) in enumerate(blocks):
            @pl.when(t == min(b + 2, slots - 1))
            def _():
                share_copy(d, p, 1 - col).wait_recv()
                across_copy(d, p, dp).start()
                near_copy(d, p, dp).start()

            @pl.when(t == min(b + 5, slots - 1))
            def _():
                across_copy(d, p, across_at).wait_recv()
                far_copy(d, p, across_at).start()

        for p in range(pairs - 1):
            @pl.when(t == 3 * p + 3 + 2 * last_place)
            def _():
                weights_ready(p)
                for d in range(2):
                    for i in range(pieces):
                        cross_copy(d, p, i, 1 - col).wait_recv()

                @pl.loop(0, tiles)
                def _(j):
                    at = pl.ds(pl.multiple_of(j * WIDE, WIDE), WIDE)
                    if p == 0:
                        total[:, at] = fold(p, every, at)
                    else:
                        total[:, at] = total[:, at] + fold(p, every, at)

    final = pairs - 1
    weights_ready(final)

    def out_copy(i):
        rows = pl.ds(i * PIECE, PIECE)
        return pltpu.make_async_copy(out.at[rows], out_hbm.at[rows], out_sem.at[i])

    for i in range(pieces):
        rows = pl.ds(i * PIECE, PIECE)
        for d in range(2):
            cross_copy(d, final, i, 1 - col).wait_recv()

        @pl.loop(0, tiles)
        def _(j):
            at = pl.ds(pl.multiple_of(j * WIDE, WIDE), WIDE)
            out[rows, at] = (total[rows, at] + fold(final, rows, at)).astype(jnp.bfloat16)

        out_copy(i).start()

    for o in range(1, rows_n):
        stat_copy(o).wait_send()
    for d in range(2):
        pos = place(d)

        @pl.when(pos < last_place)
        def _():
            @pl.loop(0, chunks)
            def _(c):
                for i in range(pieces):
                    sum_copy(d, c, i).wait_send()

        @pl.when(pos > 0)
        def _():
            @pl.loop(0, pairs)
            def _(p):
                for i in range(pieces):
                    attended_copy(d, p, i).wait_send()

    for d, p in blocks:
        share_copy(d, p, col).wait_send()
        across_copy(d, p, dp).wait_send()
        near_copy(d, p, dp).wait_send()
        far_copy(d, p, across_at).wait_send()
        for i in range(pieces):
            cross_copy(d, p, i, col).wait_send()
    for i in range(pieces):
        out_copy(i).wait()


def fused_shards(rows_n, dp_n, tokens, norm_gain, qkv_weight, out_weight):
    tokens_n, block = tokens.shape
    head_columns = qkv_weight.shape[2]
    pairs = head_columns // (2 * WIDE)
    chunks = 3 * pairs
    pieces = tokens_n // PIECE
    any_space = pl.BlockSpec(memory_space=pl.ANY)
    vmem = pl.BlockSpec(memory_space=pltpu.VMEM)
    dma = pltpu.SemaphoreType.DMA
    bf16, f32 = jnp.bfloat16, jnp.float32
    return pl.pallas_call(
        functools.partial(sublayer_kernel, rows_n, dp_n),
        out_shape=jax.ShapeDtypeStruct((tokens_n, block), bf16),
        in_specs=[any_space, vmem, any_space, any_space],
        out_specs=any_space,
        scratch_shapes=[
            pltpu.VMEM((tokens_n, block), bf16),
            pltpu.VMEM((2, chunks, block, WIDE), bf16),
            pltpu.VMEM((1, block), f32),
            pltpu.VMEM((2, tokens_n, 128), f32),
            pltpu.VMEM((rows_n, 2, 8, tokens_n), f32),
            pltpu.VMEM((tokens_n, block), bf16),
            pltpu.VMEM((2, chunks, tokens_n, WIDE), bf16),
            pltpu.VMEM((2, chunks, tokens_n, WIDE), bf16),
            pltpu.VMEM((2, 2, pairs, tokens_n, WIDE), bf16),
            pltpu.VMEM((2, 2, pairs, WIDE, block), bf16),
            pltpu.VMEM((tokens_n, block), f32),
            pltpu.VMEM((tokens_n, block), bf16),
            dma, dma((2, chunks)), dma((2, pairs)), dma((pieces,)),
            dma((rows_n,)), dma((rows_n,)),
            dma((2, chunks, pieces)), dma((2, chunks, pieces)),
            dma((2, pairs, pieces)), dma((2, pairs, pieces)),
            dma((2, pairs, pieces)), dma((2, pairs, pieces)),
            dma((2, pairs)), dma((2, pairs)), dma((2, pairs)), dma((2, pairs)),
            dma((2, pairs)), dma((2, pairs)), dma((2, pairs)), dma((2, pairs)),
        ],
        compiler_params=pltpu.CompilerParams(
            collective_id=0, has_side_effects=True, vmem_limit_bytes=52 * 1024 * 1024
        ),
    )(
        tokens, norm_gain.reshape(block // 128, 128), jnp.transpose(qkv_weight, (1, 0, 2)),
        out_weight,
    )


def solution(mesh):
    in_specs = (P("dp", "row"), P("row"), P("row", None, "col"), P("col", "row"))
    out_specs = P("dp", "row")
    rows_n, cols_n, dp_n = mesh.shape["row"], mesh.shape["col"], mesh.shape["dp"]

    def body(tokens, norm_gain, qkv_weight, out_weight):
        tokens_n, block = tokens.shape
        fits = (
            cols_n == 2 and dp_n == 4 and rows_n >= 2 and qkv_weight.shape[2] % (2 * WIDE) == 0
            and qkv_weight.shape[2] >= 4 * WIDE
            and block % WIDE == 0 and tokens_n % PIECE == 0
        )
        if fits:
            return fused_shards(rows_n, dp_n, tokens, norm_gain, qkv_weight, out_weight)
        return shards(tokens, norm_gain, qkv_weight, out_weight)

    return jax.shard_map(body, mesh=mesh, in_specs=in_specs, out_specs=out_specs, check_vma=False)
```

```python
import functools
import math

import jax
import jax.numpy as jnp
from jax import lax
from jax.experimental import pallas as pl
from jax.experimental.pallas import tpu as pltpu
from jax.sharding import PartitionSpec as P

K = 128


EPSILON = 1e-05


def attend(queries, key_rows, value_rows):
    query_total = queries.shape[0]
    head_count = queries.shape[1] // K
    scaling = 1.0 / math.sqrt(K)
    split_keys = key_rows.reshape(key_rows.shape[0], head_count, K)
    split_values = value_rows.reshape(value_rows.shape[0], head_count, K)
    split_queries = queries.reshape(query_total, head_count, K)
    scores = (
        jnp.einsum("qhd,khd->hqk", split_queries, split_keys, preferred_element_type=jnp.float32)
        * scaling
    )
    largest = jnp.max(scores, axis=2, keepdims=True)
    exponent = jnp.exp(scores - largest)
    softmax_weights = (exponent / jnp.sum(exponent, axis=2, keepdims=True)).astype(jnp.bfloat16)
    mixed = jnp.einsum(
        "hqk,khd->qhd", softmax_weights, split_values, preferred_element_type=jnp.float32
    )
    result = mixed.astype(jnp.bfloat16)
    return result.reshape(query_total, head_count * K)


def shards(tokens, norm_gain, qkv_weight, out_weight):
    row_count, block_width = tokens.shape
    full_width = block_width * lax.axis_size("row")
    values = tokens.astype(jnp.float32)
    totals, squares = lax.psum(
        (jnp.sum(values, axis=1, keepdims=True), jnp.sum(values * values, axis=1, keepdims=True)),
        "row",
    )
    average = totals / full_width
    variance = squares / full_width - average * average
    centered = values - average
    normed = (centered * lax.rsqrt(variance + EPSILON) * norm_gain).astype(jnp.bfloat16)
    head_columns = qkv_weight.shape[2]
    partial_value = jnp.dot(
        normed,
        qkv_weight.reshape(block_width, 3 * head_columns),
        preferred_element_type=jnp.float32,
    )
    summed = lax.psum(partial_value.astype(jnp.bfloat16), "row").reshape(row_count, 3, head_columns)
    attended = attend(summed[:, 0], summed[:, 1], summed[:, 2])
    partial_out = jnp.dot(attended, out_weight, preferred_element_type=jnp.float32)
    return lax.psum(partial_out.astype(jnp.bfloat16), "col")


MESH = pl.DeviceIdType.MESH
WIDE = 2 * K
ROWS = 32
EXTRA = 16
PIECE = 96
SPAN = 1
SKEW = 3
LEAD = 2
RETURN = 6
HAND = 12
HAND_ON = 24


def sublayer_kernel(
    rows_n, dp_n, tok_hbm, gain_hbm, w_hbm, wo_hbm, out,
    tok, wide_w, gain_ref, gain_row, stat_col, stats, spread_col, normed, part, gain_sum, gain_all,
    arrived, summed, attended, late_w, total,
    tok_sem, gain_sem, w_sem, late_sem, st_send, st_recv, gs_send, gs_recv, rs_send, rs_recv,
    at_send, at_recv, di_send, la_send, la_recv, lx_send, lx_recv, ly_send, ly_recv, lc_send, lc_recv,
    ld_send, ld_recv,
):
    z = lax.axis_index("row")
    col = lax.axis_index("col")
    dp = lax.axis_index("dp")
    tokens_n, block = tok.shape
    half = w_hbm.shape[2] // 2
    pairs = half // WIDE
    chunks = 3 * pairs
    pieces = tokens_n // PIECE
    units = chunks * pieces
    span = SPAN * PIECE
    spans = tokens_n // span
    tiles = block // WIDE
    quarter = WIDE // dp_n
    partner = {"col": 1 - col}
    sibling_at = dp + 1 - 2 * (dp % 2)
    across_at = (dp + 2) % dp_n
    sibling, across = {"dp": sibling_at}, {"dp": across_at}
    scaling = 1.0 / math.sqrt(K)
    last_place = rows_n - 1
    f32, bf16 = jnp.float32, jnp.bfloat16

    def weight_copy(d, c):
        pair, kind = c // 3, (c + 1) % 3
        first = pl.multiple_of(d * half + pair * WIDE, WIDE)
        return pltpu.make_async_copy(
            w_hbm.at[kind, :, pl.ds(first, WIDE)], wide_w.at[d, c], w_sem.at[d, c]
        )

    gain_load = pltpu.make_async_copy(gain_hbm, gain_ref, gain_sem)
    gain_load.start()

    def tok_copy(i):
        rows = pl.ds(pl.multiple_of(i * PIECE, PIECE), PIECE)
        return pltpu.make_async_copy(tok_hbm.at[rows], tok.at[rows], tok_sem.at[i])

    @pl.loop(0, pieces)
    def _(i):
        tok_copy(i).start()

    @pl.loop(0, chunks)
    def _(c):
        weight_copy(0, c).start()
        weight_copy(1, c).start()

    def head_columns(owner, d):
        return pl.ds(pl.multiple_of((owner * 2 + d) * WIDE, WIDE), WIDE)

    def own_copy(d, p):
        rows = pl.ds(d * half + p * WIDE, WIDE)
        return pltpu.make_async_copy(
            wo_hbm.at[rows], late_w.at[p, head_columns(col, d)], late_sem.at[d, p]
        )

    def quarter_at(owner, d, which):
        first = (owner * 2 + d) * WIDE + which * quarter
        return pl.ds(pl.multiple_of(first, quarter), quarter)

    def share_copy(d, p, owner):
        first = pl.multiple_of(d * half + p * WIDE + dp * quarter, quarter)
        return pltpu.make_async_remote_copy(
            src_ref=wo_hbm.at[pl.ds(first, quarter)],
            dst_ref=late_w.at[p, quarter_at(owner, d, dp)],
            send_sem=lx_send, recv_sem=lx_recv.at[d, p], device_id=partner,
            device_id_type=MESH,
        )

    def pass_copy(d, p, which, sends, recvs, device):
        piece = late_w.at[p, quarter_at(1 - col, d, which)]
        return pltpu.make_async_remote_copy(
            src_ref=piece, dst_ref=piece, send_sem=sends, recv_sem=recvs.at[d, p],
            device_id=device, device_id_type=MESH,
        )

    def across_copy(d, p, which):
        return pass_copy(d, p, which, ly_send, ly_recv, across)

    def near_copy(d, p, which):
        return pass_copy(d, p, which, lc_send, lc_recv, sibling)

    def far_copy(d, p, which):
        return pass_copy(d, p, which, ld_send, ld_recv, sibling)

    blocks = [(d, p) for p in range(pairs) for d in range(2)]
    for d, p in blocks:
        own_copy(d, p).start()

    barrier = pltpu.get_barrier_semaphore()
    for o in range(1, rows_n):
        pl.semaphore_signal(
            barrier, inc=1, device_id={"row": lax.rem(z + o, rows_n)}, device_id_type=MESH
        )
    for device in (partner, sibling, across):
        pl.semaphore_signal(barrier, inc=1, device_id=device, device_id_type=MESH)

    gain_load.wait()
    for j in range(block // 128):
        gain_row[0:1, j * 128:(j + 1) * 128] = gain_ref[j:j + 1, :]
    gain = gain_row[...]
    high = gain.astype(bf16).astype(f32)
    row = lax.broadcasted_iota(jnp.int32, (EXTRA, block), 0)
    normed[pl.ds(tokens_n, EXTRA), :] = jnp.where(
        row == 0, high, jnp.where(row == 1, gain - high, 0.0)
    ).astype(bf16)
    def place(d):
        return jnp.where(d == 1, z, last_place - z)

    def end_of(d):
        return jnp.where(d == 1, last_place, 0)

    def onward(d):
        return {"row": jnp.clip(jnp.where(d == 1, z + 1, z - 1), 0, last_place)}

    def back(d):
        return {"row": jnp.clip(jnp.where(d == 1, z - 1, z + 1), 0, last_place)}

    def stat_copy(which, source):
        return pltpu.make_async_remote_copy(
            src_ref=stats.at[source], dst_ref=stats.at[source], send_sem=st_send.at[which],
            recv_sem=st_recv.at[source], device_id={"row": which * last_place},
            device_id_type=MESH,
        )

    def gain_copy(d, c, source):
        return pltpu.make_async_remote_copy(
            src_ref=gain_sum.at[d, c], dst_ref=gain_all.at[source, c], send_sem=gs_send.at[d],
            recv_sem=gs_recv.at[source, c], device_id={"row": end_of(d)}, device_id_type=MESH,
        )

    def sum_copy(d, c, i):
        at = pl.ds(pl.multiple_of(i * PIECE, PIECE), PIECE)
        return pltpu.make_async_remote_copy(
            src_ref=summed.at[d, c, at], dst_ref=arrived.at[d, c, at],
            send_sem=rs_send.at[d], recv_sem=rs_recv.at[d, c, i],
            device_id=onward(d), device_id_type=MESH,
        )

    def attended_part(owner, d, p, i):
        rows = pl.ds(pl.multiple_of(i * span, span), span)
        return attended.at[p, rows, head_columns(owner, d)]

    def attended_copy(d, p, i):
        piece = attended_part(col, d, p, i)
        return pltpu.make_async_remote_copy(
            src_ref=piece, dst_ref=piece, send_sem=at_send.at[d],
            recv_sem=at_recv.at[d, p, i], device_id=back(d), device_id_type=MESH,
        )

    def direct_copy(d, p, i, o):
        piece = attended_part(col, d, p, i)
        return pltpu.make_async_remote_copy(
            src_ref=piece, dst_ref=piece, send_sem=di_send.at[o],
            recv_sem=at_recv.at[d, p, i],
            device_id={"row": jnp.clip(jnp.where(d == 1, z - o, z + o), 0, last_place)},
            device_id_type=MESH,
        )

    def cross_copy(d, p, i, owner):
        piece = attended_part(owner, d, p, i)
        return pltpu.make_async_remote_copy(
            src_ref=piece, dst_ref=piece, send_sem=la_send,
            recv_sem=la_recv.at[d, p, i], device_id=partner, device_id_type=MESH,
        )

    def attend_piece(d, p, i):
        rows = pl.ds(pl.multiple_of(i * span, span), span)
        first = (col * 2 + d) * WIDE
        for h in range(2):
            at = slice(h * K, (h + 1) * K)
            k = summed[d, 3 * p, :, at]
            v = summed[d, 3 * p + 1, :, at]
            q = summed[d, 3 * p + 2, rows, at]
            scores = lax.dot_general(
                q, k, (((1,), (1,)), ((), ())), preferred_element_type=f32
            )
            exponent = jnp.exp2(
                (scores - jnp.max(scores, axis=1, keepdims=True)) * (scaling * math.log2(math.e))
            )
            mixed = jnp.dot(exponent.astype(bf16), v, preferred_element_type=f32)
            attended[p, rows, pl.ds(pl.multiple_of(first + h * K, K), K)] = (
                mixed / jnp.sum(exponent, axis=1, keepdims=True)
            ).astype(bf16)

    def spread_statistics():
        for o in range(1, rows_n):
            stat_copy(0, lax.rem(z + o, rows_n)).wait_recv()
        mean = sum(stats[i, 0] for i in range(rows_n)) * (1.0 / rows_n)
        spread = sum(
            stats[i, 1] * (1.0 / block) + (stats[i, 0] - mean) * (stats[i, 0] - mean)
            for i in range(rows_n)
        ) * (1.0 / rows_n)
        scale = lax.rsqrt(spread + EPSILON)
        for i in range(rows_n):
            shift = (stats[i, 0] - mean) * scale
            spread_col[i] = jnp.broadcast_to(shift, (128, tokens_n)).T
        spread_col[rows_n] = jnp.broadcast_to(scale, (128, tokens_n)).T

    def weights_ready(p):
        for d in range(2):
            own_copy(d, p).wait()
            near_copy(d, p, sibling_at).wait_recv()
            far_copy(d, p, (sibling_at + 2) % dp_n).wait_recv()

    def pair_ready(p):
        weights_ready(p)
        for d in range(2):
            for i in range(spans):
                cross_copy(d, p, i, 1 - col).wait_recv()

    def fold(p, rows, at):
        return jnp.dot(attended[p, rows, :], late_w[p, :, at], preferred_element_type=f32)

    nearer = jnp.where(z < last_place - z, 1, 0)
    starts = (z == 0) | (z == last_place)

    def centre(i):
        tok_copy(i).wait()

        @pl.loop(0, PIECE // ROWS)
        def _(j):
            at = pl.ds(pl.multiple_of(i * PIECE + j * ROWS, ROWS), ROWS)
            x = tok[at, :].astype(f32)
            mean = jnp.sum(x, axis=1, keepdims=True) * (1.0 / block)
            away = x - mean
            square = jnp.sum(away * away, axis=1, keepdims=True)
            normed[at, :] = (away * gain_row[...]).astype(bf16)
            stat_col[0, at, :] = jnp.broadcast_to(mean, (ROWS, 128))
            stat_col[1, at, :] = jnp.broadcast_to(square, (ROWS, 128))

    def first_piece(i):
        rows = pl.ds(pl.multiple_of(i * PIECE, PIECE), PIECE)
        summed[nearer, 0, rows] = jnp.dot(
            normed[rows, :], wide_w[nearer, 0], preferred_element_type=f32
        ).astype(bf16)

    centre(0)

    @pl.when(starts)
    def _():
        weight_copy(nearer, 0).wait()
        first_piece(0)

    pl.semaphore_wait(barrier, rows_n + 2)

    @pl.when(starts)
    def _():
        sum_copy(nearer, 0, 0).start()

    @pl.loop(0, pairs)
    def _(p):
        share_copy(0, p, col).start()
        share_copy(1, p, col).start()

    @pl.loop(1, pieces)
    def _(i):
        centre(i)

        @pl.when(starts)
        def _():
            first_piece(i)
            sum_copy(nearer, 0, i).start()

    @pl.when(starts)
    def _():
        value = jnp.dot(
            normed[pl.ds(tokens_n, EXTRA), :], wide_w[nearer, 0], preferred_element_type=f32
        )
        gain_sum[nearer, 0] = value[0:1] + value[1:2]
        gain_copy(nearer, 0, z).start()

    def offset(pos):
        return jnp.where(pos > 0, LEAD + SKEW * pos, -pieces)

    end_offset = LEAD + SKEW * last_place
    slots = units + end_offset + RETURN + SKEW * last_place
    every = pl.ds(0, tokens_n)

    def fold_pair(p):
        pair_ready(p)
        for j in range(tiles // 2):
            at = slice(j * 2 * WIDE, (j + 1) * 2 * WIDE)
            value = fold(p, every, at)
            total[:, at] = value if p == 0 else total[:, at] + value

    stat_slot = jnp.where(starts, 0, LEAD + SKEW + 1)

    @pl.loop(0, slots)
    def _(t):
        @pl.when(t == stat_slot)
        def _():
            stats[z, 0] = stat_col[0].T[0:1]
            stats[z, 1] = stat_col[1].T[0:1]
            for which in range(2):
                @pl.when(z != which * last_place)
                def _():
                    stat_copy(which, z).start()

        @pl.when((t == end_offset - 1) & starts)
        def _():
            spread_statistics()

        for k in range(2):
            d = nearer if k == 0 else 1 - nearer
            pos = place(d)
            u = t - offset(pos)
            c, i = u // pieces, u % pieces

            @pl.when((u >= 0) & (u < units))
            def _():
                rows = pl.ds(pl.multiple_of(i * PIECE, PIECE), PIECE)

                @pl.when(i == 0)
                def _():
                    weight_copy(d, c).wait()
                    value = jnp.dot(normed[...], wide_w[d, c], preferred_element_type=f32)
                    part[d] = value[0:tokens_n]
                    gain_value = value[tokens_n:tokens_n + 1] + value[tokens_n + 1:tokens_n + 2]

                    @pl.when(pos < last_place)
                    def _():
                        gain_sum[d, c] = gain_value
                        gain_copy(d, c, z).start()

                    @pl.when(pos == last_place)
                    def _():
                        gain_all[z, c] = gain_value
                        for o in range(1, rows_n):
                            gain_copy(d, c, lax.rem(z + o, rows_n)).wait_recv()

                @pl.when(pos == 0)
                def _():
                    summed[d, c, rows] = part[d, rows].astype(bf16)

                @pl.when(pos > 0)
                def _():
                    sum_copy(d, c, i).wait_recv()

                @pl.when((pos > 0) & (pos < last_place))
                def _():
                    summed[d, c, rows] = (part[d, rows] + arrived[d, c, rows].astype(f32)).astype(bf16)

                @pl.when(pos < last_place)
                def _():
                    sum_copy(d, c, i).start()

                @pl.when(pos == last_place)
                def _():
                    scale = spread_col[rows_n, rows]
                    for h in range(2):
                        lanes = slice(h * 128, (h + 1) * 128)
                        whole = part[d, rows, lanes] + arrived[d, c, rows, lanes].astype(f32)
                        whole = whole * scale
                        for source in range(rows_n):
                            whole = whole + spread_col[source, rows] * gain_all[source, c, :, lanes]
                        summed[d, c, rows, lanes] = whole.astype(bf16)

                @pl.when((pos == last_place) & (c % 3 == 2) & (i % SPAN == SPAN - 1))
                def _():
                    p, s = c // 3, i // SPAN
                    attend_piece(d, p, s)

                    @pl.when(u < units - 1)
                    def _():
                        attended_copy(d, p, s).start()

                    @pl.when(u == units - 1)
                    def _():
                        for o in range(last_place, 0, -1):
                            direct_copy(d, p, s, o).start()

                    cross_copy(d, p, s, col).start()

        for k in range(2):
            d = 1 - nearer if k == 0 else nearer
            pos = place(d)
            u = t - end_offset - RETURN - SKEW * (last_place - pos)
            c, i = u // pieces, u % pieces
            p = c // 3

            @pl.when(
                (pos < last_place) & (u >= 0) & (u < units) & (c % 3 == 2) & (i % SPAN == SPAN - 1)
            )
            def _():
                s = i // SPAN
                attended_copy(d, p, s).wait_recv()

                @pl.when((pos > 0) & (u < units - 1))
                def _():
                    attended_copy(d, p, s).start()

                cross_copy(d, p, s, col).start()

        @pl.when((t >= HAND) & (t < HAND + pieces * len(blocks)) & ((t - HAND) % pieces == 0))
        def _():
            b = (t - HAND) // pieces
            d, p = b % 2, b // 2
            share_copy(d, p, 1 - col).wait_recv()
            across_copy(d, p, dp).start()
            near_copy(d, p, dp).start()

        @pl.when(
            (t >= HAND_ON) & (t < HAND_ON + pieces * len(blocks)) & ((t - HAND_ON) % pieces == 0)
        )
        def _():
            b = (t - HAND_ON) // pieces
            d, p = b % 2, b // 2
            across_copy(d, p, across_at).wait_recv()
            far_copy(d, p, across_at).start()

        @pl.when(t == units + end_offset)
        def _():
            for p in range(pairs - 2):
                fold_pair(p)

    final = pairs - 1
    fold_pair(final - 1)
    weights_ready(final)

    for i in range(spans):
        rows = pl.ds(i * span, span)
        for d in range(2):
            cross_copy(d, final, i, 1 - col).wait_recv()
        for j in range(tiles // 2):
            at = slice(j * 2 * WIDE, (j + 1) * 2 * WIDE)
            out[rows, at] = (total[rows, at] + fold(final, rows, at)).astype(bf16)

    def sent(source, sem):
        pltpu.make_async_remote_copy(
            src_ref=source, dst_ref=source, send_sem=sem, recv_sem=lx_recv.at[0, 0],
            device_id=partner, device_id_type=MESH,
        ).wait_send()

    for which in range(2):
        @pl.when(z != which * last_place)
        def _():
            stat_copy(which, z).wait_send()
    for d in range(2):
        pos = place(d)

        @pl.when(pos < last_place)
        def _():
            sent(gain_sum.at[d], gs_send.at[d])
            sent(summed.at[d], rs_send.at[d])

        @pl.when(pos > 0)
        def _():
            sent(wide_w.at[0, 0, pl.ds(0, pairs * tokens_n - span)], at_send.at[d])

        @pl.when(pos == last_place)
        def _():
            for o in range(1, rows_n):
                direct_copy(d, final, spans - 1, o).wait_send()

    sent(summed.at[0, pl.ds(0, 2 * pairs)], la_send)
    for sem in (lx_send, ly_send, lc_send, ld_send):
        sent(late_w.at[0, pl.ds(0, 2 * pairs * quarter)], sem)


def fused_shards(rows_n, dp_n, tokens, norm_gain, qkv_weight, out_weight):
    tokens_n, block = tokens.shape
    pairs = qkv_weight.shape[2] // (2 * WIDE)
    chunks = 3 * pairs
    pieces, spans = tokens_n // PIECE, tokens_n // (SPAN * PIECE)
    any_space = pl.BlockSpec(memory_space=pl.ANY)
    vmem = pl.BlockSpec(memory_space=pltpu.VMEM)
    hbm = pl.BlockSpec(memory_space=pltpu.HBM)
    dma = pltpu.SemaphoreType.DMA
    bf16, f32 = jnp.bfloat16, jnp.float32
    return pl.pallas_call(
        functools.partial(sublayer_kernel, rows_n, dp_n),
        out_shape=pltpu.VMEM((tokens_n, block), bf16),
        in_specs=[any_space, hbm, any_space, any_space],
        out_specs=vmem,
        scratch_shapes=[
            pltpu.VMEM((tokens_n, block), bf16),
            pltpu.VMEM((2, chunks, block, WIDE), bf16),
            pltpu.VMEM((block // 128, 128), f32),
            pltpu.VMEM((1, block), f32),
            pltpu.VMEM((2, tokens_n, 128), f32),
            pltpu.VMEM((rows_n, 2, 1, tokens_n), f32),
            pltpu.VMEM((rows_n + 1, tokens_n, 128), f32),
            pltpu.VMEM((tokens_n + EXTRA, block), bf16),
            pltpu.VMEM((2, tokens_n, WIDE), f32),
            pltpu.VMEM((2, chunks, 1, WIDE), f32),
            pltpu.VMEM((rows_n, chunks, 1, WIDE), f32),
            pltpu.VMEM((2, chunks, tokens_n, WIDE), bf16),
            pltpu.VMEM((2, chunks, tokens_n, WIDE), bf16),
            pltpu.VMEM((pairs, tokens_n, 4 * WIDE), bf16),
            pltpu.VMEM((pairs, 4 * WIDE, block), bf16),
            pltpu.VMEM((tokens_n, block), f32),
            dma((pieces,)), dma, dma((2, chunks)), dma((2, pairs)),
            dma((2,)), dma((rows_n,)), dma((2,)), dma((rows_n, chunks)),
            dma((2,)), dma((2, chunks, pieces)),
            dma((2,)), dma((2, pairs, spans)), dma((rows_n,)),
            dma, dma((2, pairs, spans)),
            dma, dma((2, pairs)), dma, dma((2, pairs)),
            dma, dma((2, pairs)), dma, dma((2, pairs)),
        ],
        compiler_params=pltpu.CompilerParams(
            collective_id=0, has_side_effects=True, vmem_limit_bytes=65800000
        ),
    )(
        tokens, norm_gain.reshape(block // 128, 128), jnp.transpose(qkv_weight, (1, 0, 2)),
        out_weight,
    )


def solution(mesh):
    in_specs = (P("dp", "row"), P("row"), P("row", None, "col"), P("col", "row"))
    out_specs = P("dp", "row")
    rows_n, cols_n, dp_n = mesh.shape["row"], mesh.shape["col"], mesh.shape["dp"]

    def body(tokens, norm_gain, qkv_weight, out_weight):
        tokens_n, block = tokens.shape
        fits = (
            cols_n == 2 and dp_n == 4 and rows_n >= 2 and qkv_weight.shape[2] % (2 * WIDE) == 0
            and qkv_weight.shape[2] >= 4 * WIDE
            and block % (2 * WIDE) == 0 and tokens_n % (SPAN * PIECE) == 0
            and (qkv_weight.shape[2] // (2 * WIDE)) * tokens_n <= block
        )
        if fits:
            return fused_shards(rows_n, dp_n, tokens, norm_gain, qkv_weight, out_weight)
        return shards(tokens, norm_gain, qkv_weight, out_weight)

    return jax.shard_map(body, mesh=mesh, in_specs=in_specs, out_specs=out_specs, check_vma=False)
```

```python
import functools
import math

import jax
import jax.numpy as jnp
from jax import lax
from jax.experimental import pallas as pl
from jax.experimental.pallas import tpu as pltpu
from jax.sharding import PartitionSpec as P

K = 128


EPSILON = 1e-05


def attend(queries, key_rows, value_rows):
    query_total = queries.shape[0]
    head_count = queries.shape[1] // K
    scaling = 1.0 / math.sqrt(K)
    split_keys = key_rows.reshape(key_rows.shape[0], head_count, K)
    split_values = value_rows.reshape(value_rows.shape[0], head_count, K)
    split_queries = queries.reshape(query_total, head_count, K)
    scores = (
        jnp.einsum("qhd,khd->hqk", split_queries, split_keys, preferred_element_type=jnp.float32)
        * scaling
    )
    largest = jnp.max(scores, axis=2, keepdims=True)
    exponent = jnp.exp(scores - largest)
    softmax_weights = (exponent / jnp.sum(exponent, axis=2, keepdims=True)).astype(jnp.bfloat16)
    mixed = jnp.einsum(
        "hqk,khd->qhd", softmax_weights, split_values, preferred_element_type=jnp.float32
    )
    result = mixed.astype(jnp.bfloat16)
    return result.reshape(query_total, head_count * K)


def shards(tokens, norm_gain, qkv_weight, out_weight):
    row_count, block_width = tokens.shape
    full_width = block_width * lax.axis_size("row")
    values = tokens.astype(jnp.float32)
    totals, squares = lax.psum(
        (jnp.sum(values, axis=1, keepdims=True), jnp.sum(values * values, axis=1, keepdims=True)),
        "row",
    )
    average = totals / full_width
    variance = squares / full_width - average * average
    centered = values - average
    normed = (centered * lax.rsqrt(variance + EPSILON) * norm_gain).astype(jnp.bfloat16)
    head_columns = qkv_weight.shape[2]
    partial_value = jnp.dot(
        normed,
        qkv_weight.reshape(block_width, 3 * head_columns),
        preferred_element_type=jnp.float32,
    )
    summed = lax.psum(partial_value.astype(jnp.bfloat16), "row").reshape(row_count, 3, head_columns)
    attended = attend(summed[:, 0], summed[:, 1], summed[:, 2])
    partial_out = jnp.dot(attended, out_weight, preferred_element_type=jnp.float32)
    return lax.psum(partial_out.astype(jnp.bfloat16), "col")


MESH = pl.DeviceIdType.MESH
WIDE = 2 * K
ROWS = 32
EXTRA = 16
PIECE = 96
SKEW = 3
LEAD = 1
HAND = 12
HAND_ON = 24


def stream_starts(pairs, pieces, lag):
    place, unit, starts, asked = 0, 0, [], {}
    while unit < 3 * pairs * pieces:
        following = len(starts)
        if following < pairs - 2 and place >= asked.get(following, place + 1) + lag:
            starts.append(place)
            place += pieces
            continue
        if unit % (3 * pieces) == 2 * pieces:
            asked[unit // (3 * pieces)] = place
        unit += 1
        place += 1
    for pair in range(len(starts), pairs):
        place = max(place, asked[pair] + lag)
        starts.append(place)
        place += pieces
    return starts


def sublayer_kernel(
    rows_n, dp_n, tok_hbm, gain_hbm, w_hbm, wo_hbm, out,
    tok, wide_w, gain_ref, gain_row, stat_col, stats, spread_col, normed, part, gain_sum, gain_all,
    arrived, summed, attended, late_w, total,
    tok_sem, gain_sem, w_sem, late_sem, st_send, st_recv, gs_send, gs_recv, rs_send, rs_recv,
    at_send, at_recv, di_send, la_send, la_recv, lx_send, lx_recv, ly_send, ly_recv, lc_send, lc_recv,
    ld_send, ld_recv,
):
    z = lax.axis_index("row")
    col = lax.axis_index("col")
    dp = lax.axis_index("dp")
    tokens_n, block = tok.shape
    half = w_hbm.shape[2] // 2
    pairs = half // WIDE
    chunks = 3 * pairs
    pieces = tokens_n // PIECE
    units = chunks * pieces
    tiles = block // WIDE
    quarter = WIDE // dp_n
    partner = {"col": 1 - col}
    sibling_at = dp + 1 - 2 * (dp % 2)
    across_at = (dp + 2) % dp_n
    sibling, across = {"dp": sibling_at}, {"dp": across_at}
    scaling = 1.0 / math.sqrt(K)
    last_place = rows_n - 1
    f32, bf16 = jnp.float32, jnp.bfloat16

    def weight_copy(d, c):
        pair, kind = c // 3, (c + 1) % 3
        first = pl.multiple_of(d * half + pair * WIDE, WIDE)
        return pltpu.make_async_copy(
            w_hbm.at[kind, :, pl.ds(first, WIDE)], wide_w.at[d, c], w_sem.at[d, c]
        )

    gain_load = pltpu.make_async_copy(gain_hbm, gain_ref, gain_sem)
    gain_load.start()

    def tok_copy(i):
        rows = pl.ds(pl.multiple_of(i * PIECE, PIECE), PIECE)
        return pltpu.make_async_copy(tok_hbm.at[rows], tok.at[rows], tok_sem.at[i])

    @pl.loop(0, pieces)
    def _(i):
        tok_copy(i).start()

    @pl.loop(0, chunks)
    def _(c):
        weight_copy(0, c).start()
        weight_copy(1, c).start()

    def head_columns(owner, d):
        return pl.ds(pl.multiple_of((owner * 2 + d) * WIDE, WIDE), WIDE)

    def own_copy(d, p):
        rows = pl.ds(d * half + p * WIDE, WIDE)
        return pltpu.make_async_copy(
            wo_hbm.at[rows], late_w.at[p, head_columns(col, d)], late_sem.at[d, p]
        )

    def quarter_at(owner, d, which):
        first = (owner * 2 + d) * WIDE + which * quarter
        return pl.ds(pl.multiple_of(first, quarter), quarter)

    def share_copy(d, p, owner):
        first = pl.multiple_of(d * half + p * WIDE + dp * quarter, quarter)
        return pltpu.make_async_remote_copy(
            src_ref=wo_hbm.at[pl.ds(first, quarter)],
            dst_ref=late_w.at[p, quarter_at(owner, d, dp)],
            send_sem=lx_send, recv_sem=lx_recv.at[d, p], device_id=partner,
            device_id_type=MESH,
        )

    def pass_copy(d, p, which, sends, recvs, device):
        piece = late_w.at[p, quarter_at(1 - col, d, which)]
        return pltpu.make_async_remote_copy(
            src_ref=piece, dst_ref=piece, send_sem=sends, recv_sem=recvs.at[d, p],
            device_id=device, device_id_type=MESH,
        )

    def across_copy(d, p, which):
        return pass_copy(d, p, which, ly_send, ly_recv, across)

    def near_copy(d, p, which):
        return pass_copy(d, p, which, lc_send, lc_recv, sibling)

    def far_copy(d, p, which):
        return pass_copy(d, p, which, ld_send, ld_recv, sibling)

    blocks = [(d, p) for p in range(pairs) for d in range(2)]
    for d, p in blocks:
        own_copy(d, p).start()

    barrier = pltpu.get_barrier_semaphore()
    for o in range(1, rows_n):
        pl.semaphore_signal(
            barrier, inc=1, device_id={"row": lax.rem(z + o, rows_n)}, device_id_type=MESH
        )
    for device in (partner, sibling, across):
        pl.semaphore_signal(barrier, inc=1, device_id=device, device_id_type=MESH)

    gain_load.wait()
    for j in range(block // 128):
        gain_row[0:1, j * 128:(j + 1) * 128] = gain_ref[j:j + 1, :]
    gain = gain_row[...]
    high = gain.astype(bf16).astype(f32)
    row = lax.broadcasted_iota(jnp.int32, (EXTRA, block), 0)
    normed[pl.ds(tokens_n, EXTRA), :] = jnp.where(
        row == 0, high, jnp.where(row == 1, gain - high, 0.0)
    ).astype(bf16)
    def place(d):
        return jnp.where(d == 1, z, last_place - z)

    def end_of(d):
        return jnp.where(d == 1, last_place, 0)

    def onward(d):
        return {"row": jnp.clip(jnp.where(d == 1, z + 1, z - 1), 0, last_place)}

    def back(d):
        return {"row": jnp.clip(jnp.where(d == 1, z - 1, z + 1), 0, last_place)}

    def stat_copy(which, source):
        return pltpu.make_async_remote_copy(
            src_ref=stats.at[source], dst_ref=stats.at[source], send_sem=st_send.at[which],
            recv_sem=st_recv.at[source], device_id={"row": which * last_place},
            device_id_type=MESH,
        )

    def gain_copy(d, c, source):
        return pltpu.make_async_remote_copy(
            src_ref=gain_sum.at[d, c], dst_ref=gain_all.at[source, c], send_sem=gs_send.at[d],
            recv_sem=gs_recv.at[source, c], device_id={"row": end_of(d)}, device_id_type=MESH,
        )

    def sum_copy(d, c, i):
        at = pl.ds(pl.multiple_of(i * PIECE, PIECE), PIECE)
        return pltpu.make_async_remote_copy(
            src_ref=summed.at[d, c, at], dst_ref=arrived.at[d, c, at],
            send_sem=rs_send.at[d], recv_sem=rs_recv.at[d, c, i],
            device_id=onward(d), device_id_type=MESH,
        )

    def attended_part(owner, d, p, i):
        rows = pl.ds(pl.multiple_of(i * PIECE, PIECE), PIECE)
        return attended.at[p, rows, head_columns(owner, d)]

    def attended_copy(d, p, i):
        piece = attended_part(col, d, p, i)
        return pltpu.make_async_remote_copy(
            src_ref=piece, dst_ref=piece, send_sem=at_send.at[d],
            recv_sem=at_recv.at[d, p, i], device_id=back(d), device_id_type=MESH,
        )

    def direct_copy(d, p, i, o):
        piece = attended_part(col, d, p, i)
        return pltpu.make_async_remote_copy(
            src_ref=piece, dst_ref=piece, send_sem=di_send.at[o],
            recv_sem=at_recv.at[d, p, i],
            device_id={"row": jnp.clip(jnp.where(d == 1, z - o, z + o), 0, last_place)},
            device_id_type=MESH,
        )

    def cross_copy(d, p, i, owner):
        piece = attended_part(owner, d, p, i)
        return pltpu.make_async_remote_copy(
            src_ref=piece, dst_ref=piece, send_sem=la_send,
            recv_sem=la_recv.at[d, p, i], device_id=partner, device_id_type=MESH,
        )

    def attend_piece(d, p, i):
        rows = pl.ds(pl.multiple_of(i * PIECE, PIECE), PIECE)
        first = (col * 2 + d) * WIDE
        for h in range(2):
            at = slice(h * K, (h + 1) * K)
            k = summed[d, 3 * p, :, at]
            v = summed[d, 3 * p + 1, :, at]
            q = summed[d, 3 * p + 2, rows, at]
            scores = lax.dot_general(
                q, k, (((1,), (1,)), ((), ())), preferred_element_type=f32
            )
            exponent = jnp.exp2(
                (scores - jnp.max(scores, axis=1, keepdims=True)) * (scaling * math.log2(math.e))
            )
            mixed = jnp.dot(exponent.astype(bf16), v, preferred_element_type=f32)
            attended[p, rows, pl.ds(pl.multiple_of(first + h * K, K), K)] = (
                mixed / jnp.sum(exponent, axis=1, keepdims=True)
            ).astype(bf16)

    def spread_statistics():
        for o in range(1, rows_n):
            stat_copy(0, lax.rem(z + o, rows_n)).wait_recv()
        mean = sum(stats[i, 0] for i in range(rows_n)) * (1.0 / rows_n)
        spread = sum(
            stats[i, 1] * (1.0 / block) + (stats[i, 0] - mean) * (stats[i, 0] - mean)
            for i in range(rows_n)
        ) * (1.0 / rows_n)
        scale = lax.rsqrt(spread + EPSILON)
        for i in range(rows_n):
            shift = (stats[i, 0] - mean) * scale
            spread_col[i] = jnp.broadcast_to(shift, (128, tokens_n)).T
        spread_col[rows_n] = jnp.broadcast_to(scale, (128, tokens_n)).T

    def weights_ready(p):
        for d in range(2):
            own_copy(d, p).wait()
            near_copy(d, p, sibling_at).wait_recv()
            far_copy(d, p, (sibling_at + 2) % dp_n).wait_recv()

    def pair_ready(p):
        weights_ready(p)
        for d in range(2):
            for i in range(pieces):
                cross_copy(d, p, i, 1 - col).wait_recv()

    def fold(p, rows, at):
        return jnp.dot(attended[p, rows, :], late_w[p, :, at], preferred_element_type=f32)

    nearer = jnp.where(z < last_place - z, 1, 0)
    starts = (z == 0) | (z == last_place)

    def centre(i):
        tok_copy(i).wait()

        @pl.loop(0, PIECE // ROWS)
        def _(j):
            at = pl.ds(pl.multiple_of(i * PIECE + j * ROWS, ROWS), ROWS)
            x = tok[at, :].astype(f32)
            mean = jnp.sum(x, axis=1, keepdims=True) * (1.0 / block)
            away = x - mean
            square = jnp.sum(away * away, axis=1, keepdims=True)
            normed[at, :] = (away * gain_row[...]).astype(bf16)
            stat_col[0, at, :] = jnp.broadcast_to(mean, (ROWS, 128))
            stat_col[1, at, :] = jnp.broadcast_to(square, (ROWS, 128))

    def first_piece(i):
        rows = pl.ds(pl.multiple_of(i * PIECE, PIECE), PIECE)
        summed[nearer, 0, rows] = jnp.dot(
            normed[rows, :], wide_w[nearer, 0], preferred_element_type=f32
        ).astype(bf16)

    centre(0)

    @pl.when(starts)
    def _():
        weight_copy(nearer, 0).wait()
        first_piece(0)

    pl.semaphore_wait(barrier, rows_n + 2)

    @pl.when(starts)
    def _():
        sum_copy(nearer, 0, 0).start()

    @pl.loop(0, pairs)
    def _(p):
        share_copy(0, p, col).start()
        share_copy(1, p, col).start()

    @pl.loop(1, pieces)
    def _(i):
        centre(i)

        @pl.when(starts)
        def _():
            first_piece(i)
            sum_copy(nearer, 0, i).start()

    @pl.when(starts)
    def _():
        value = jnp.dot(
            normed[pl.ds(tokens_n, EXTRA), :], wide_w[nearer, 0], preferred_element_type=f32
        )
        gain_sum[nearer, 0] = value[0:1] + value[1:2]
        gain_copy(nearer, 0, z).start()

    def offset(pos):
        return jnp.where(pos > 0, LEAD + SKEW * pos, -pieces)

    end_offset = LEAD + SKEW * last_place
    begins = stream_starts(pairs, pieces, end_offset + pieces + 1)
    slots = begins[-1] + pieces + end_offset
    every = pl.ds(0, tokens_n)

    def fold_pair(p):
        pair_ready(p)
        for j in range(tiles // 2):
            at = slice(j * 2 * WIDE, (j + 1) * 2 * WIDE)
            value = fold(p, every, at)
            total[:, at] = value if p == 0 else total[:, at] + value

    stat_slot = jnp.where(starts, 0, LEAD + SKEW + 1)

    @pl.loop(0, slots)
    def _(t):
        @pl.when(t == stat_slot)
        def _():
            stats[z, 0] = stat_col[0].T[0:1]
            stats[z, 1] = stat_col[1].T[0:1]
            for which in range(2):
                @pl.when(z != which * last_place)
                def _():
                    stat_copy(which, z).start()

        @pl.when((t == end_offset - 1) & starts)
        def _():
            spread_statistics()

        for k in range(2):
            d = nearer if k == 0 else 1 - nearer
            pos = place(d)
            n = t - offset(pos)
            u = n
            returns = False
            back_pair, back_piece = 0, 0
            for p, begin in enumerate(begins):
                inside = (n >= begin) & (n < begin + pieces)
                returns = returns | inside
                back_pair = jnp.where(inside, p, back_pair)
                back_piece = jnp.where(inside, n - begin, back_piece)
                u = jnp.where(n >= begin + pieces, u - pieces, u)
            c, i = u // pieces, u % pieces

            @pl.when((u >= 0) & (u < units) & jnp.logical_not(returns))
            def _():
                rows = pl.ds(pl.multiple_of(i * PIECE, PIECE), PIECE)

                @pl.when(i == 0)
                def _():
                    weight_copy(d, c).wait()
                    value = jnp.dot(normed[...], wide_w[d, c], preferred_element_type=f32)
                    part[d] = value[0:tokens_n]
                    gain_value = value[tokens_n:tokens_n + 1] + value[tokens_n + 1:tokens_n + 2]

                    @pl.when(pos < last_place)
                    def _():
                        gain_sum[d, c] = gain_value
                        gain_copy(d, c, z).start()

                    @pl.when(pos == last_place)
                    def _():
                        gain_all[z, c] = gain_value
                        for o in range(1, rows_n):
                            gain_copy(d, c, lax.rem(z + o, rows_n)).wait_recv()

                @pl.when(pos == 0)
                def _():
                    summed[d, c, rows] = part[d, rows].astype(bf16)

                @pl.when(pos > 0)
                def _():
                    sum_copy(d, c, i).wait_recv()

                @pl.when((pos > 0) & (pos < last_place))
                def _():
                    summed[d, c, rows] = (part[d, rows] + arrived[d, c, rows].astype(f32)).astype(bf16)

                @pl.when(pos < last_place)
                def _():
                    sum_copy(d, c, i).start()

                @pl.when(pos == last_place)
                def _():
                    scale = spread_col[rows_n, rows]
                    for h in range(2):
                        lanes = slice(h * 128, (h + 1) * 128)
                        whole = part[d, rows, lanes] + arrived[d, c, rows, lanes].astype(f32)
                        whole = whole * scale
                        for source in range(rows_n):
                            whole = whole + spread_col[source, rows] * gain_all[source, c, :, lanes]
                        summed[d, c, rows, lanes] = whole.astype(bf16)

                @pl.when((pos == last_place) & (c % 3 == 2))
                def _():
                    attend_piece(d, c // 3, i)
                    cross_copy(d, c // 3, i, col).start()

            @pl.when(returns)
            def _():
                p, s, other = back_pair, back_piece, 1 - d
                direct = (p == pairs - 1) & (s == pieces - 1)

                @pl.when(pos > 0)
                def _():
                    attended_copy(other, p, s).wait_recv()

                @pl.when((pos < last_place) & jnp.logical_not(direct))
                def _():
                    attended_copy(other, p, s).start()

                @pl.when((pos == 0) & direct)
                def _():
                    for o in range(last_place, 0, -1):
                        direct_copy(other, p, s, o).start()

                @pl.when(pos > 0)
                def _():
                    cross_copy(other, p, s, col).start()

        @pl.when((t >= HAND) & (t < HAND + pieces * len(blocks)) & ((t - HAND) % pieces == 0))
        def _():
            b = (t - HAND) // pieces
            d, p = b % 2, b // 2
            share_copy(d, p, 1 - col).wait_recv()
            across_copy(d, p, dp).start()
            near_copy(d, p, dp).start()

        @pl.when(
            (t >= HAND_ON) & (t < HAND_ON + pieces * len(blocks)) & ((t - HAND_ON) % pieces == 0)
        )
        def _():
            b = (t - HAND_ON) // pieces
            d, p = b % 2, b // 2
            across_copy(d, p, across_at).wait_recv()
            far_copy(d, p, across_at).start()

        @pl.when(t == begins[pairs - 2] + pieces + end_offset)
        def _():
            for p in range(pairs - 2):
                fold_pair(p)

    final = pairs - 1
    fold_pair(final - 1)
    weights_ready(final)

    for i in range(pieces):
        rows = pl.ds(i * PIECE, PIECE)
        for d in range(2):
            cross_copy(d, final, i, 1 - col).wait_recv()
        for j in range(tiles // 2):
            at = slice(j * 2 * WIDE, (j + 1) * 2 * WIDE)
            out[rows, at] = (total[rows, at] + fold(final, rows, at)).astype(bf16)

    def sent(source, sem):
        pltpu.make_async_remote_copy(
            src_ref=source, dst_ref=source, send_sem=sem, recv_sem=lx_recv.at[0, 0],
            device_id=partner, device_id_type=MESH,
        ).wait_send()

    for which in range(2):
        @pl.when(z != which * last_place)
        def _():
            stat_copy(which, z).wait_send()
    for d in range(2):
        pos = place(d)

        @pl.when(pos < last_place)
        def _():
            sent(gain_sum.at[d], gs_send.at[d])
            sent(summed.at[d], rs_send.at[d])

        @pl.when(pos > 0)
        def _():
            sent(wide_w.at[0, 0, pl.ds(0, pairs * tokens_n - PIECE)], at_send.at[d])

        @pl.when(pos == last_place)
        def _():
            for o in range(1, rows_n):
                direct_copy(d, final, pieces - 1, o).wait_send()

    sent(summed.at[0, pl.ds(0, 2 * pairs)], la_send)
    for sem in (lx_send, ly_send, lc_send, ld_send):
        sent(late_w.at[0, pl.ds(0, 2 * pairs * quarter)], sem)


def fused_shards(rows_n, dp_n, tokens, norm_gain, qkv_weight, out_weight):
    tokens_n, block = tokens.shape
    pairs = qkv_weight.shape[2] // (2 * WIDE)
    chunks = 3 * pairs
    pieces = tokens_n // PIECE
    any_space = pl.BlockSpec(memory_space=pl.ANY)
    vmem = pl.BlockSpec(memory_space=pltpu.VMEM)
    hbm = pl.BlockSpec(memory_space=pltpu.HBM)
    dma = pltpu.SemaphoreType.DMA
    bf16, f32 = jnp.bfloat16, jnp.float32
    return pl.pallas_call(
        functools.partial(sublayer_kernel, rows_n, dp_n),
        out_shape=pltpu.VMEM((tokens_n, block), bf16),
        in_specs=[any_space, hbm, any_space, any_space],
        out_specs=vmem,
        scratch_shapes=[
            pltpu.VMEM((tokens_n, block), bf16),
            pltpu.VMEM((2, chunks, block, WIDE), bf16),
            pltpu.VMEM((block // 128, 128), f32),
            pltpu.VMEM((1, block), f32),
            pltpu.VMEM((2, tokens_n, 128), f32),
            pltpu.VMEM((rows_n, 2, 1, tokens_n), f32),
            pltpu.VMEM((rows_n + 1, tokens_n, 128), f32),
            pltpu.VMEM((tokens_n + EXTRA, block), bf16),
            pltpu.VMEM((2, tokens_n, WIDE), f32),
            pltpu.VMEM((2, chunks, 1, WIDE), f32),
            pltpu.VMEM((rows_n, chunks, 1, WIDE), f32),
            pltpu.VMEM((2, chunks, tokens_n, WIDE), bf16),
            pltpu.VMEM((2, chunks, tokens_n, WIDE), bf16),
            pltpu.VMEM((pairs, tokens_n, 4 * WIDE), bf16),
            pltpu.VMEM((pairs, 4 * WIDE, block), bf16),
            pltpu.VMEM((tokens_n, block), f32),
            dma((pieces,)), dma, dma((2, chunks)), dma((2, pairs)),
            dma((2,)), dma((rows_n,)), dma((2,)), dma((rows_n, chunks)),
            dma((2,)), dma((2, chunks, pieces)),
            dma((2,)), dma((2, pairs, pieces)), dma((rows_n,)),
            dma, dma((2, pairs, pieces)),
            dma, dma((2, pairs)), dma, dma((2, pairs)),
            dma, dma((2, pairs)), dma, dma((2, pairs)),
        ],
        compiler_params=pltpu.CompilerParams(
            collective_id=0, has_side_effects=True, vmem_limit_bytes=65800000
        ),
    )(
        tokens, norm_gain.reshape(block // 128, 128), jnp.transpose(qkv_weight, (1, 0, 2)),
        out_weight,
    )


def solution(mesh):
    in_specs = (P("dp", "row"), P("row"), P("row", None, "col"), P("col", "row"))
    out_specs = P("dp", "row")
    rows_n, cols_n, dp_n = mesh.shape["row"], mesh.shape["col"], mesh.shape["dp"]

    def body(tokens, norm_gain, qkv_weight, out_weight):
        tokens_n, block = tokens.shape
        fits = (
            cols_n == 2 and dp_n == 4 and rows_n >= 2 and qkv_weight.shape[2] % (2 * WIDE) == 0
            and qkv_weight.shape[2] >= 4 * WIDE
            and block % (2 * WIDE) == 0 and tokens_n % PIECE == 0
            and (qkv_weight.shape[2] // (2 * WIDE)) * tokens_n <= block
        )
        if fits:
            return fused_shards(rows_n, dp_n, tokens, norm_gain, qkv_weight, out_weight)
        return shards(tokens, norm_gain, qkv_weight, out_weight)

    return jax.shard_map(body, mesh=mesh, in_specs=in_specs, out_specs=out_specs, check_vma=False)
```

```python
import functools
import math

import jax
import jax.numpy as jnp
from jax import lax
from jax.experimental import pallas as pl
from jax.experimental.pallas import tpu as pltpu
from jax.sharding import PartitionSpec as P

K = 128


EPSILON = 1e-05


def attend(queries, key_rows, value_rows):
    query_total = queries.shape[0]
    head_count = queries.shape[1] // K
    scaling = 1.0 / math.sqrt(K)
    split_keys = key_rows.reshape(key_rows.shape[0], head_count, K)
    split_values = value_rows.reshape(value_rows.shape[0], head_count, K)
    split_queries = queries.reshape(query_total, head_count, K)
    scores = (
        jnp.einsum("qhd,khd->hqk", split_queries, split_keys, preferred_element_type=jnp.float32)
        * scaling
    )
    largest = jnp.max(scores, axis=2, keepdims=True)
    exponent = jnp.exp(scores - largest)
    softmax_weights = (exponent / jnp.sum(exponent, axis=2, keepdims=True)).astype(jnp.bfloat16)
    mixed = jnp.einsum(
        "hqk,khd->qhd", softmax_weights, split_values, preferred_element_type=jnp.float32
    )
    result = mixed.astype(jnp.bfloat16)
    return result.reshape(query_total, head_count * K)


def shards(tokens, norm_gain, qkv_weight, out_weight):
    row_count, block_width = tokens.shape
    full_width = block_width * lax.axis_size("row")
    values = tokens.astype(jnp.float32)
    totals, squares = lax.psum(
        (jnp.sum(values, axis=1, keepdims=True), jnp.sum(values * values, axis=1, keepdims=True)),
        "row",
    )
    average = totals / full_width
    variance = squares / full_width - average * average
    centered = values - average
    normed = (centered * lax.rsqrt(variance + EPSILON) * norm_gain).astype(jnp.bfloat16)
    head_columns = qkv_weight.shape[2]
    partial_value = jnp.dot(
        normed,
        qkv_weight.reshape(block_width, 3 * head_columns),
        preferred_element_type=jnp.float32,
    )
    summed = lax.psum(partial_value.astype(jnp.bfloat16), "row").reshape(row_count, 3, head_columns)
    attended = attend(summed[:, 0], summed[:, 1], summed[:, 2])
    partial_out = jnp.dot(attended, out_weight, preferred_element_type=jnp.float32)
    return lax.psum(partial_out.astype(jnp.bfloat16), "col")


MESH = pl.DeviceIdType.MESH
WIDE = 2 * K
ROWS = 32
EXTRA = 16
PIECE = 96
GROUP = 2
DIRECT = 1
SKEW = 3
LEAD = 1
HAND = 16
HAND_ON = 28


def stream_starts(pairs, pieces, lag):
    place, unit, starts, asked = 0, 0, [], {}
    while unit < 3 * pairs * pieces:
        following = len(starts)
        if following < pairs - 2 and place >= asked.get(following, place + 1) + lag:
            starts.append(place)
            place += pieces
            continue
        if unit % (3 * pieces) == 2 * pieces:
            asked[unit // (3 * pieces)] = place
        unit += 1
        place += 1
    for pair in range(len(starts), pairs):
        place = max(place, asked[pair] + lag)
        starts.append(place)
        place += pieces
    return starts


def sublayer_kernel(
    rows_n, dp_n, tok_hbm, gain_hbm, w_hbm, wo_hbm, out,
    tok, wide_w, gain_ref, gain_row, stat_col, stats, spread_col, normed, part, gain_sum, gain_all,
    arrived, summed, attended, late_w, total,
    tok_sem, gain_sem, w_sem, late_sem, st_send, st_recv, gs_send, gs_recv, rs_send, rs_recv,
    at_send, at_recv, di_send, lp_recv, la_send, la_recv, lx_send, lx_recv, ly_send, ly_recv, lc_send, lc_recv,
    ld_send, ld_recv,
):
    z = lax.axis_index("row")
    col = lax.axis_index("col")
    dp = lax.axis_index("dp")
    tokens_n, block = tok.shape
    half = w_hbm.shape[2] // 2
    pairs = half // WIDE
    chunks = 3 * pairs
    pieces = tokens_n // PIECE
    units = chunks * pieces
    tiles = block // WIDE
    quarter = WIDE // dp_n
    partner = {"col": 1 - col}
    sibling_at = dp + 1 - 2 * (dp % 2)
    across_at = (dp + 2) % dp_n
    sibling, across = {"dp": sibling_at}, {"dp": across_at}
    scaling = 1.0 / math.sqrt(K)
    last_place = rows_n - 1
    f32, bf16 = jnp.float32, jnp.bfloat16

    def weight_copy(d, c):
        pair, kind = c // 3, (c + 1) % 3
        first = pl.multiple_of(d * half + pair * WIDE, WIDE)
        return pltpu.make_async_copy(
            w_hbm.at[kind, :, pl.ds(first, WIDE)], wide_w.at[d, c], w_sem.at[d, c]
        )

    gain_load = pltpu.make_async_copy(gain_hbm, gain_ref, gain_sem)
    gain_load.start()

    def tok_copy(i):
        rows = pl.ds(pl.multiple_of(i * PIECE, PIECE), PIECE)
        return pltpu.make_async_copy(tok_hbm.at[rows], tok.at[rows], tok_sem.at[i])

    @pl.loop(0, pieces)
    def _(i):
        tok_copy(i).start()

    @pl.loop(0, chunks)
    def _(c):
        weight_copy(0, c).start()
        weight_copy(1, c).start()

    def head_columns(owner, d):
        return pl.ds(pl.multiple_of((owner * 2 + d) * WIDE, WIDE), WIDE)

    def own_copy(d, p):
        rows = pl.ds(d * half + p * WIDE, WIDE)
        return pltpu.make_async_copy(
            wo_hbm.at[rows], late_w.at[p, head_columns(col, d)], late_sem.at[p]
        )

    def quarter_at(owner, d, which):
        first = (owner * 2 + d) * WIDE + which * quarter
        return pl.ds(pl.multiple_of(first, quarter), quarter)

    def share_copy(d, p, owner):
        first = pl.multiple_of(d * half + p * WIDE + dp * quarter, quarter)
        return pltpu.make_async_remote_copy(
            src_ref=wo_hbm.at[pl.ds(first, quarter)],
            dst_ref=late_w.at[p, quarter_at(owner, d, dp)],
            send_sem=lx_send, recv_sem=lx_recv.at[p], device_id=partner,
            device_id_type=MESH,
        )

    def pass_copy(d, p, which, sends, recvs, device):
        piece = late_w.at[p, quarter_at(1 - col, d, which)]
        return pltpu.make_async_remote_copy(
            src_ref=piece, dst_ref=piece, send_sem=sends, recv_sem=recvs.at[p],
            device_id=device, device_id_type=MESH,
        )

    def across_copy(d, p, which):
        return pass_copy(d, p, which, ly_send, ly_recv, across)

    def near_copy(d, p, which):
        return pass_copy(d, p, which, lc_send, lc_recv, sibling)

    def far_copy(d, p, which):
        return pass_copy(d, p, which, ld_send, ld_recv, sibling)

    def whole(source, sem):
        return pltpu.make_async_remote_copy(
            src_ref=source, dst_ref=source, send_sem=sem, recv_sem=sem,
            device_id=partner, device_id_type=MESH,
        )

    def sent(source, sem):
        whole(source, sem).wait_send()

    def landed(target, sem):
        whole(target, sem).wait_recv()

    @pl.loop(0, pairs)
    def _(p):
        own_copy(0, p).start()
        own_copy(1, p).start()

    barrier = pltpu.get_barrier_semaphore()
    for o in range(1, rows_n):
        pl.semaphore_signal(
            barrier, inc=1, device_id={"row": lax.rem(z + o, rows_n)}, device_id_type=MESH
        )
    for device in (partner, sibling, across):
        pl.semaphore_signal(barrier, inc=1, device_id=device, device_id_type=MESH)

    gain_load.wait()
    for j in range(block // 128):
        gain_row[0:1, j * 128:(j + 1) * 128] = gain_ref[j:j + 1, :]
    gain = gain_row[...]
    high = gain.astype(bf16).astype(f32)
    row = lax.broadcasted_iota(jnp.int32, (EXTRA, block), 0)
    normed[pl.ds(tokens_n, EXTRA), :] = jnp.where(
        row == 0, high, jnp.where(row == 1, gain - high, 0.0)
    ).astype(bf16)
    def place(d):
        return jnp.where(d == 1, z, last_place - z)

    def end_of(d):
        return jnp.where(d == 1, last_place, 0)

    def onward(d):
        return {"row": jnp.clip(jnp.where(d == 1, z + 1, z - 1), 0, last_place)}

    def back(d):
        return {"row": jnp.clip(jnp.where(d == 1, z - 1, z + 1), 0, last_place)}

    def stat_copy(which, source):
        return pltpu.make_async_remote_copy(
            src_ref=stats.at[source], dst_ref=stats.at[source], send_sem=st_send.at[which],
            recv_sem=st_recv.at[source], device_id={"row": which * last_place},
            device_id_type=MESH,
        )

    def gain_copy(d, c, source):
        return pltpu.make_async_remote_copy(
            src_ref=gain_sum.at[d, c], dst_ref=gain_all.at[c, source], send_sem=gs_send.at[d],
            recv_sem=gs_recv.at[c], device_id={"row": end_of(d)}, device_id_type=MESH,
        )

    def sum_copy(d, c, i):
        at = pl.ds(pl.multiple_of(i * PIECE, PIECE), PIECE)
        return pltpu.make_async_remote_copy(
            src_ref=summed.at[d, c, at], dst_ref=arrived.at[d, c, at],
            send_sem=rs_send.at[d], recv_sem=rs_recv.at[d, c, i],
            device_id=onward(d), device_id_type=MESH,
        )

    def attended_part(owner, d, p, i):
        rows = pl.ds(pl.multiple_of(i * PIECE, PIECE), PIECE)
        return attended.at[p, rows, head_columns(owner, d)]

    def attended_copy(d, p, i):
        piece = attended_part(col, d, p, i)
        return pltpu.make_async_remote_copy(
            src_ref=piece, dst_ref=piece, send_sem=at_send.at[d],
            recv_sem=at_recv.at[d, p, i], device_id=back(d), device_id_type=MESH,
        )

    def direct_copy(d, p, i, o):
        piece = attended_part(col, d, p, i)
        return pltpu.make_async_remote_copy(
            src_ref=piece, dst_ref=piece, send_sem=di_send,
            recv_sem=at_recv.at[d, p, i],
            device_id={"row": jnp.clip(jnp.where(d == 1, z - o, z + o), 0, last_place)},
            device_id_type=MESH,
        )

    def cross_copy(d, p, i, owner, recv_sem):
        piece = attended_part(owner, d, p, i)
        return pltpu.make_async_remote_copy(
            src_ref=piece, dst_ref=piece, send_sem=la_send,
            recv_sem=recv_sem, device_id=partner, device_id_type=MESH,
        )

    def cross_over(d, p, i):
        @pl.when(p < pairs - 1)
        def _():
            cross_copy(d, p, i, col, lp_recv.at[jnp.minimum(p, pairs - 2)]).start()

        @pl.when(p == pairs - 1)
        def _():
            cross_copy(d, p, i, col, la_recv.at[d, i]).start()

    def attend_piece(d, p, i):
        rows = pl.ds(pl.multiple_of(i * PIECE, PIECE), PIECE)
        first = (col * 2 + d) * WIDE
        for h in range(2):
            at = slice(h * K, (h + 1) * K)
            k = summed[d, 3 * p, :, at]
            v = summed[d, 3 * p + 1, :, at]
            q = summed[d, 3 * p + 2, rows, at]
            scores = lax.dot_general(
                q, k, (((1,), (1,)), ((), ())), preferred_element_type=f32
            )
            exponent = jnp.exp2(
                (scores - jnp.max(scores, axis=1, keepdims=True)) * (scaling * math.log2(math.e))
            )
            mixed = jnp.dot(exponent.astype(bf16), v, preferred_element_type=f32)
            attended[p, rows, pl.ds(pl.multiple_of(first + h * K, K), K)] = (
                mixed / jnp.sum(exponent, axis=1, keepdims=True)
            ).astype(bf16)

    def spread_statistics():
        for o in range(1, rows_n):
            stat_copy(0, lax.rem(z + o, rows_n)).wait_recv()
        mean = sum(stats[i, 0] for i in range(rows_n)) * (1.0 / rows_n)
        spread = sum(
            stats[i, 1] * (1.0 / block) + (stats[i, 0] - mean) * (stats[i, 0] - mean)
            for i in range(rows_n)
        ) * (1.0 / rows_n)
        scale = lax.rsqrt(spread + EPSILON)
        for i in range(rows_n):
            shift = (stats[i, 0] - mean) * scale
            spread_col[i] = jnp.broadcast_to(shift, (128, tokens_n)).T
        spread_col[rows_n] = jnp.broadcast_to(scale, (128, tokens_n)).T

    def weights_ready(p):
        rows = late_w.at[p, pl.ds(0, 2 * WIDE)]
        pltpu.make_async_copy(rows, rows, late_sem.at[p]).wait()
        for recvs in (lc_recv, ld_recv):
            landed(late_w.at[p, pl.ds(0, 2 * quarter)], recvs.at[p])

    def pair_ready(p):
        weights_ready(p)
        landed(summed.at[0, pl.ds(0, 2)], lp_recv.at[p])

    def fold(p, rows, at):
        return jnp.dot(attended[p, rows, :], late_w[p, :, at], preferred_element_type=f32)

    nearer = jnp.where(z < last_place - z, 1, 0)
    starts = (z == 0) | (z == last_place)

    def centre(i):
        tok_copy(i).wait()

        @pl.loop(0, PIECE // ROWS)
        def _(j):
            at = pl.ds(pl.multiple_of(i * PIECE + j * ROWS, ROWS), ROWS)
            x = tok[at, :].astype(f32)
            mean = jnp.sum(x, axis=1, keepdims=True) * (1.0 / block)
            away = x - mean
            square = jnp.sum(away * away, axis=1, keepdims=True)
            normed[at, :] = (away * gain_row[...]).astype(bf16)
            stat_col[0, at, :] = jnp.broadcast_to(mean, (ROWS, 128))
            stat_col[1, at, :] = jnp.broadcast_to(square, (ROWS, 128))

    def first_piece(i):
        rows = pl.ds(pl.multiple_of(i * PIECE, PIECE), PIECE)
        summed[nearer, 0, rows] = jnp.dot(
            normed[rows, :], wide_w[nearer, 0], preferred_element_type=f32
        ).astype(bf16)

    centre(0)

    @pl.when(starts)
    def _():
        weight_copy(nearer, 0).wait()
        first_piece(0)

    pl.semaphore_wait(barrier, rows_n + 2)

    @pl.when(starts)
    def _():
        sum_copy(nearer, 0, 0).start()

    @pl.loop(0, pairs)
    def _(p):
        share_copy(0, p, col).start()
        share_copy(1, p, col).start()

    @pl.loop(1, pieces)
    def _(i):
        centre(i)

        @pl.when(starts)
        def _():
            first_piece(i)
            sum_copy(nearer, 0, i).start()

    @pl.when(starts)
    def _():
        value = jnp.dot(
            normed[pl.ds(tokens_n, EXTRA), :], wide_w[nearer, 0], preferred_element_type=f32
        )
        gain_sum[nearer, 0] = value[0:1] + value[1:2]
        gain_copy(nearer, 0, z).start()

    def offset(pos):
        return jnp.where(pos > 0, LEAD + SKEW * pos, -pieces)

    end_offset = LEAD + SKEW * last_place
    begins = stream_starts(pairs, pieces, end_offset + pieces + 1)
    slots = begins[-1] + pieces + end_offset
    every = pl.ds(0, tokens_n)

    def fold_pair(p):
        pair_ready(p)
        for j in range(tiles // 2):
            at = slice(j * 2 * WIDE, (j + 1) * 2 * WIDE)
            value = fold(p, every, at)
            total[:, at] = value if p == 0 else total[:, at] + value

    stat_slot = jnp.where(starts, 0, LEAD + SKEW + 1)

    @pl.loop(0, slots)
    def _(t):
        @pl.when(t == stat_slot)
        def _():
            stats[z, 0] = stat_col[0].T[0:1]
            stats[z, 1] = stat_col[1].T[0:1]
            for which in range(2):
                @pl.when(z != which * last_place)
                def _():
                    stat_copy(which, z).start()

        @pl.when((t == end_offset - 1) & starts)
        def _():
            spread_statistics()

        for k in range(2):
            d = nearer if k == 0 else 1 - nearer
            pos = place(d)
            n = t - offset(pos)
            u = n
            returns = False
            back_pair, back_piece = 0, 0
            for p, begin in enumerate(begins):
                inside = (n >= begin) & (n < begin + pieces)
                returns = returns | inside
                back_pair = jnp.where(inside, p, back_pair)
                back_piece = jnp.where(inside, n - begin, back_piece)
                u = jnp.where(n >= begin + pieces, u - pieces, u)
            c, i = u // pieces, u % pieces

            @pl.when((u >= 0) & (u < units) & jnp.logical_not(returns))
            def _():
                rows = pl.ds(pl.multiple_of(i * PIECE, PIECE), PIECE)

                @pl.when(i == 0)
                def _():
                    weight_copy(d, c).wait()
                    value = jnp.dot(normed[...], wide_w[d, c], preferred_element_type=f32)
                    part[d] = value[0:tokens_n]
                    gain_value = value[tokens_n:tokens_n + 1] + value[tokens_n + 1:tokens_n + 2]

                    @pl.when(pos < last_place)
                    def _():
                        gain_sum[d, c] = gain_value
                        gain_copy(d, c, z).start()

                    @pl.when(pos == last_place)
                    def _():
                        gain_all[c, z] = gain_value
                        landed(gain_all.at[c, pl.ds(0, last_place)], gs_recv.at[c])

                @pl.when(pos == 0)
                def _():
                    summed[d, c, rows] = part[d, rows].astype(bf16)

                @pl.when(pos > 0)
                def _():
                    sum_copy(d, c, i).wait_recv()

                @pl.when((pos > 0) & (pos < last_place))
                def _():
                    summed[d, c, rows] = (part[d, rows] + arrived[d, c, rows].astype(f32)).astype(bf16)

                @pl.when(pos < last_place)
                def _():
                    sum_copy(d, c, i).start()

                @pl.when(pos == last_place)
                def _():
                    scale = spread_col[rows_n, rows]
                    for h in range(2):
                        lanes = slice(h * 128, (h + 1) * 128)
                        whole = part[d, rows, lanes] + arrived[d, c, rows, lanes].astype(f32)
                        whole = whole * scale
                        for source in range(rows_n):
                            whole = whole + spread_col[source, rows] * gain_all[c, source, :, lanes]
                        summed[d, c, rows, lanes] = whole.astype(bf16)

                @pl.when((pos == last_place) & (c % 3 == 2))
                def _():
                    attend_piece(d, c // 3, i)
                    cross_over(d, c // 3, i)

            @pl.when(returns)
            def _():
                p, other = back_pair, 1 - d
                turned = (p == pairs - 1) & (pos == last_place)
                s = jnp.where(turned, (back_piece + pieces - DIRECT) % pieces, back_piece)
                direct = (p == pairs - 1) & (s >= pieces - DIRECT)

                @pl.when(pos > 0)
                def _():
                    attended_copy(other, p, s).wait_recv()

                @pl.when((pos < last_place) & jnp.logical_not(direct))
                def _():
                    attended_copy(other, p, s).start()

                @pl.when((pos == 0) & direct)
                def _():
                    for o in range(last_place, 0, -1):
                        direct_copy(other, p, s, o).start()

                @pl.when(pos > 0)
                def _():
                    cross_over(other, p, s)

        @pl.when((t >= HAND) & (t < HAND + 2 * pieces * pairs) & ((t - HAND) % (2 * pieces) == 0))
        def _():
            p = (t - HAND) // (2 * pieces)
            landed(late_w.at[p, pl.ds(0, 2 * quarter)], lx_recv.at[p])
            for d in range(2):
                across_copy(d, p, dp).start()
                near_copy(d, p, dp).start()

        @pl.when(
            (t >= HAND_ON) & (t < HAND_ON + 2 * pieces * pairs)
            & ((t - HAND_ON) % (2 * pieces) == 0)
        )
        def _():
            p = (t - HAND_ON) // (2 * pieces)
            landed(late_w.at[p, pl.ds(0, 2 * quarter)], ly_recv.at[p])
            for d in range(2):
                far_copy(d, p, across_at).start()

        @pl.when(t == begins[pairs - 2] + pieces + end_offset)
        def _():
            for p in range(pairs - 2):
                fold_pair(p)

    final = pairs - 1
    fold_pair(final - 1)
    weights_ready(final)

    def fold_owner(rows, at, owner):
        heads = pl.ds(pl.multiple_of(owner * 2 * WIDE, 2 * WIDE), 2 * WIDE)
        return jnp.dot(
            attended[final, rows, heads], late_w[final, heads, at], preferred_element_type=f32
        )

    for j in range(tiles // 2):
        at = slice(j * 2 * WIDE, (j + 1) * 2 * WIDE)
        total[:, at] = total[:, at] + fold_owner(every, at, col)

    for first in range(0, pieces, GROUP):
        group = range(first, min(first + GROUP, pieces))
        rows = slice(first * PIECE, (group[-1] + 1) * PIECE)
        for d in range(2):
            for i in group:
                cross_copy(d, final, i, 1 - col, la_recv.at[d, i]).wait_recv()
        for j in range(tiles // 2):
            at = slice(j * 2 * WIDE, (j + 1) * 2 * WIDE)
            out[rows, at] = (total[rows, at] + fold_owner(rows, at, 1 - col)).astype(bf16)

    for which in range(2):
        @pl.when(z != which * last_place)
        def _():
            stat_copy(which, z).wait_send()
    for d in range(2):
        pos = place(d)

        @pl.when(pos < last_place)
        def _():
            sent(gain_sum.at[d], gs_send.at[d])
            sent(summed.at[d], rs_send.at[d])

        @pl.when(pos > 0)
        def _():
            sent(wide_w.at[0, 0, pl.ds(0, pairs * tokens_n - DIRECT * PIECE)], at_send.at[d])

        @pl.when(pos == last_place)
        def _():
            sent(wide_w.at[0, 0, pl.ds(0, last_place * DIRECT * PIECE)], di_send)

    sent(summed.at[0, pl.ds(0, 2 * pairs)], la_send)
    for sem in (lx_send, ly_send, lc_send, ld_send):
        sent(late_w.at[0, pl.ds(0, 2 * pairs * quarter)], sem)


def fused_shards(rows_n, dp_n, tokens, norm_gain, qkv_weight, out_weight):
    tokens_n, block = tokens.shape
    pairs = qkv_weight.shape[2] // (2 * WIDE)
    chunks = 3 * pairs
    pieces = tokens_n // PIECE
    any_space = pl.BlockSpec(memory_space=pl.ANY)
    vmem = pl.BlockSpec(memory_space=pltpu.VMEM)
    hbm = pl.BlockSpec(memory_space=pltpu.HBM)
    dma = pltpu.SemaphoreType.DMA
    bf16, f32 = jnp.bfloat16, jnp.float32
    return pl.pallas_call(
        functools.partial(sublayer_kernel, rows_n, dp_n),
        out_shape=pltpu.VMEM((tokens_n, block), bf16),
        in_specs=[any_space, hbm, any_space, any_space],
        out_specs=vmem,
        scratch_shapes=[
            pltpu.VMEM((tokens_n, block), bf16),
            pltpu.VMEM((2, chunks, block, WIDE), bf16),
            pltpu.VMEM((block // 128, 128), f32),
            pltpu.VMEM((1, block), f32),
            pltpu.VMEM((2, tokens_n, 128), f32),
            pltpu.VMEM((rows_n, 2, 1, tokens_n), f32),
            pltpu.VMEM((rows_n + 1, tokens_n, 128), f32),
            pltpu.VMEM((tokens_n + EXTRA, block), bf16),
            pltpu.VMEM((2, tokens_n, WIDE), f32),
            pltpu.VMEM((2, chunks, 1, WIDE), f32),
            pltpu.VMEM((chunks, rows_n, 1, WIDE), f32),
            pltpu.VMEM((2, chunks, tokens_n, WIDE), bf16),
            pltpu.VMEM((2, chunks, tokens_n, WIDE), bf16),
            pltpu.VMEM((pairs, tokens_n, 4 * WIDE), bf16),
            pltpu.VMEM((pairs, 4 * WIDE, block), bf16),
            pltpu.VMEM((tokens_n, block), f32),
            dma((pieces,)), dma, dma((2, chunks)), dma((pairs,)),
            dma((2,)), dma((rows_n,)), dma((2,)), dma((chunks,)),
            dma((2,)), dma((2, chunks, pieces)),
            dma((2,)), dma((2, pairs, pieces)), dma, dma((pairs - 1,)),
            dma, dma((2, pieces)), dma, dma((pairs,)), dma, dma((pairs,)),
            dma, dma((pairs,)), dma, dma((pairs,)),
        ],
        compiler_params=pltpu.CompilerParams(
            collective_id=0, has_side_effects=True, vmem_limit_bytes=65800000
        ),
    )(
        tokens, norm_gain.reshape(block // 128, 128), jnp.transpose(qkv_weight, (1, 0, 2)),
        out_weight,
    )


def solution(mesh):
    in_specs = (P("dp", "row"), P("row"), P("row", None, "col"), P("col", "row"))
    out_specs = P("dp", "row")
    rows_n, cols_n, dp_n = mesh.shape["row"], mesh.shape["col"], mesh.shape["dp"]

    def body(tokens, norm_gain, qkv_weight, out_weight):
        tokens_n, block = tokens.shape
        fits = (
            cols_n == 2 and dp_n == 4 and rows_n >= 2 and qkv_weight.shape[2] % (2 * WIDE) == 0
            and qkv_weight.shape[2] >= 4 * WIDE
            and block % (2 * WIDE) == 0 and tokens_n % PIECE == 0
            and (qkv_weight.shape[2] // (2 * WIDE)) * tokens_n <= block
            and (rows_n - 1) * DIRECT * PIECE <= block and tokens_n > DIRECT * PIECE
        )
        if fits:
            return fused_shards(rows_n, dp_n, tokens, norm_gain, qkv_weight, out_weight)
        return shards(tokens, norm_gain, qkv_weight, out_weight)

    return jax.shard_map(body, mesh=mesh, in_specs=in_specs, out_specs=out_specs, check_vma=False)
```

```python
import functools
import math

import jax
import jax.numpy as jnp
from jax import lax
from jax.experimental import pallas as pl
from jax.experimental.pallas import tpu as pltpu
from jax.sharding import PartitionSpec as P

K = 128


EPSILON = 1e-05


def attend(queries, key_rows, value_rows):
    query_total = queries.shape[0]
    head_count = queries.shape[1] // K
    scaling = 1.0 / math.sqrt(K)
    split_keys = key_rows.reshape(key_rows.shape[0], head_count, K)
    split_values = value_rows.reshape(value_rows.shape[0], head_count, K)
    split_queries = queries.reshape(query_total, head_count, K)
    scores = (
        jnp.einsum("qhd,khd->hqk", split_queries, split_keys, preferred_element_type=jnp.float32)
        * scaling
    )
    largest = jnp.max(scores, axis=2, keepdims=True)
    exponent = jnp.exp(scores - largest)
    softmax_weights = (exponent / jnp.sum(exponent, axis=2, keepdims=True)).astype(jnp.bfloat16)
    mixed = jnp.einsum(
        "hqk,khd->qhd", softmax_weights, split_values, preferred_element_type=jnp.float32
    )
    result = mixed.astype(jnp.bfloat16)
    return result.reshape(query_total, head_count * K)


def shards(tokens, norm_gain, qkv_weight, out_weight):
    row_count, block_width = tokens.shape
    full_width = block_width * lax.axis_size("row")
    values = tokens.astype(jnp.float32)
    totals, squares = lax.psum(
        (jnp.sum(values, axis=1, keepdims=True), jnp.sum(values * values, axis=1, keepdims=True)),
        "row",
    )
    average = totals / full_width
    variance = squares / full_width - average * average
    centered = values - average
    normed = (centered * lax.rsqrt(variance + EPSILON) * norm_gain).astype(jnp.bfloat16)
    head_columns = qkv_weight.shape[2]
    partial_value = jnp.dot(
        normed,
        qkv_weight.reshape(block_width, 3 * head_columns),
        preferred_element_type=jnp.float32,
    )
    summed = lax.psum(partial_value.astype(jnp.bfloat16), "row").reshape(row_count, 3, head_columns)
    attended = attend(summed[:, 0], summed[:, 1], summed[:, 2])
    partial_out = jnp.dot(attended, out_weight, preferred_element_type=jnp.float32)
    return lax.psum(partial_out.astype(jnp.bfloat16), "col")


MESH = pl.DeviceIdType.MESH
WIDE = 2 * K
ROWS = 32
EXTRA = 16
PIECE = 96
GROUP = 2
DIRECT = 1
EARLY = 3
SKEW = 3
LEAD = 1
HAND = 16
HAND_ON = 28


def stream_blocks(pairs, pieces, lag):
    place, unit, blocks, asked = 0, 0, [], {}
    early = min(EARLY, pieces)
    while unit < 3 * pairs * pieces:
        following = len(blocks)
        if early and following < pairs - 2 and place >= asked.get(following, place + 1) + lag:
            blocks.append((following, 0, early, place))
            place += early
            continue
        if unit % (3 * pieces) == 2 * pieces:
            asked[unit // (3 * pieces)] = place
        unit += 1
        place += 1
    gone = len(blocks)
    for pair in range(pairs):
        first = early if pair < gone else 0
        if first < pieces:
            place = max(place, asked[pair] + first + lag)
            blocks.append((pair, first, pieces - first, place))
            place += pieces - first
    return blocks


def sublayer_kernel(
    rows_n, dp_n, tok_hbm, gain_hbm, w_hbm, wo_hbm, out,
    tok, wide_w, gain_ref, gain_row, stat_col, stats, spread_col, normed, part, gain_sum, gain_all,
    arrived, summed, attended, late_w, total,
    tok_sem, gain_sem, w_sem, late_sem, st_send, st_recv, gs_send, gs_recv, rs_send, rs_recv,
    at_send, at_recv, di_send, lp_recv, la_send, la_recv, lx_send, lx_recv, ly_send, ly_recv, lc_send, lc_recv,
    ld_send, ld_recv,
):
    z = lax.axis_index("row")
    col = lax.axis_index("col")
    dp = lax.axis_index("dp")
    tokens_n, block = tok.shape
    half = w_hbm.shape[2] // 2
    pairs = half // WIDE
    chunks = 3 * pairs
    pieces = tokens_n // PIECE
    units = chunks * pieces
    tiles = block // WIDE
    quarter = WIDE // dp_n
    partner = {"col": 1 - col}
    sibling_at = dp + 1 - 2 * (dp % 2)
    across_at = (dp + 2) % dp_n
    sibling, across = {"dp": sibling_at}, {"dp": across_at}
    scaling = 1.0 / math.sqrt(K)
    last_place = rows_n - 1
    f32, bf16 = jnp.float32, jnp.bfloat16

    def weight_copy(d, c):
        pair, kind = c // 3, (c + 1) % 3
        first = pl.multiple_of(d * half + pair * WIDE, WIDE)
        return pltpu.make_async_copy(
            w_hbm.at[kind, :, pl.ds(first, WIDE)], wide_w.at[d, c], w_sem.at[d, c]
        )

    gain_load = pltpu.make_async_copy(gain_hbm, gain_ref, gain_sem)
    gain_load.start()

    def tok_copy(i):
        rows = pl.ds(pl.multiple_of(i * PIECE, PIECE), PIECE)
        return pltpu.make_async_copy(tok_hbm.at[rows], tok.at[rows], tok_sem.at[i])

    @pl.loop(0, pieces)
    def _(i):
        tok_copy(i).start()

    @pl.loop(0, chunks)
    def _(c):
        weight_copy(0, c).start()
        weight_copy(1, c).start()

    def head_columns(owner, d):
        return pl.ds(pl.multiple_of((owner * 2 + d) * WIDE, WIDE), WIDE)

    def own_copy(d, p):
        rows = pl.ds(d * half + p * WIDE, WIDE)
        return pltpu.make_async_copy(
            wo_hbm.at[rows], late_w.at[p, head_columns(col, d)], late_sem.at[p]
        )

    def quarter_at(owner, d, which):
        first = (owner * 2 + d) * WIDE + which * quarter
        return pl.ds(pl.multiple_of(first, quarter), quarter)

    def share_copy(d, p, owner):
        first = pl.multiple_of(d * half + p * WIDE + dp * quarter, quarter)
        return pltpu.make_async_remote_copy(
            src_ref=wo_hbm.at[pl.ds(first, quarter)],
            dst_ref=late_w.at[p, quarter_at(owner, d, dp)],
            send_sem=lx_send, recv_sem=lx_recv.at[p], device_id=partner,
            device_id_type=MESH,
        )

    def pass_copy(d, p, which, sends, recvs, device):
        piece = late_w.at[p, quarter_at(1 - col, d, which)]
        return pltpu.make_async_remote_copy(
            src_ref=piece, dst_ref=piece, send_sem=sends, recv_sem=recvs.at[p],
            device_id=device, device_id_type=MESH,
        )

    def across_copy(d, p, which):
        return pass_copy(d, p, which, ly_send, ly_recv, across)

    def near_copy(d, p, which):
        return pass_copy(d, p, which, lc_send, lc_recv, sibling)

    def far_copy(d, p, which):
        return pass_copy(d, p, which, ld_send, ld_recv, sibling)

    def whole(source, sem):
        return pltpu.make_async_remote_copy(
            src_ref=source, dst_ref=source, send_sem=sem, recv_sem=sem,
            device_id=partner, device_id_type=MESH,
        )

    def sent(source, sem):
        whole(source, sem).wait_send()

    def landed(target, sem):
        whole(target, sem).wait_recv()

    @pl.loop(0, pairs)
    def _(p):
        own_copy(0, p).start()
        own_copy(1, p).start()

    barrier = pltpu.get_barrier_semaphore()
    for o in range(1, rows_n):
        pl.semaphore_signal(
            barrier, inc=1, device_id={"row": lax.rem(z + o, rows_n)}, device_id_type=MESH
        )
    for device in (partner, sibling, across):
        pl.semaphore_signal(barrier, inc=1, device_id=device, device_id_type=MESH)

    gain_load.wait()
    for j in range(block // 128):
        gain_row[0:1, j * 128:(j + 1) * 128] = gain_ref[j:j + 1, :]
    gain = gain_row[...]
    high = gain.astype(bf16).astype(f32)
    row = lax.broadcasted_iota(jnp.int32, (EXTRA, block), 0)
    normed[pl.ds(tokens_n, EXTRA), :] = jnp.where(
        row == 0, high, jnp.where(row == 1, gain - high, 0.0)
    ).astype(bf16)
    def place(d):
        return jnp.where(d == 1, z, last_place - z)

    def end_of(d):
        return jnp.where(d == 1, last_place, 0)

    def onward(d):
        return {"row": jnp.clip(jnp.where(d == 1, z + 1, z - 1), 0, last_place)}

    def back(d):
        return {"row": jnp.clip(jnp.where(d == 1, z - 1, z + 1), 0, last_place)}

    def stat_copy(which, source):
        return pltpu.make_async_remote_copy(
            src_ref=stats.at[source], dst_ref=stats.at[source], send_sem=st_send.at[which],
            recv_sem=st_recv.at[source], device_id={"row": which * last_place},
            device_id_type=MESH,
        )

    def gain_copy(d, c, source):
        return pltpu.make_async_remote_copy(
            src_ref=gain_sum.at[d, c], dst_ref=gain_all.at[c, source], send_sem=gs_send.at[d],
            recv_sem=gs_recv.at[c], device_id={"row": end_of(d)}, device_id_type=MESH,
        )

    def sum_copy(d, c, i):
        at = pl.ds(pl.multiple_of(i * PIECE, PIECE), PIECE)
        return pltpu.make_async_remote_copy(
            src_ref=summed.at[d, c, at], dst_ref=arrived.at[d, c, at],
            send_sem=rs_send.at[d], recv_sem=rs_recv.at[d, c, i],
            device_id=onward(d), device_id_type=MESH,
        )

    def attended_part(owner, d, p, i):
        rows = pl.ds(pl.multiple_of(i * PIECE, PIECE), PIECE)
        return attended.at[p, rows, head_columns(owner, d)]

    def attended_copy(d, p, i):
        piece = attended_part(col, d, p, i)
        return pltpu.make_async_remote_copy(
            src_ref=piece, dst_ref=piece, send_sem=at_send.at[d],
            recv_sem=at_recv.at[d, p, i], device_id=back(d), device_id_type=MESH,
        )

    def direct_copy(d, p, i, o):
        piece = attended_part(col, d, p, i)
        return pltpu.make_async_remote_copy(
            src_ref=piece, dst_ref=piece, send_sem=di_send,
            recv_sem=at_recv.at[d, p, i],
            device_id={"row": jnp.clip(jnp.where(d == 1, z - o, z + o), 0, last_place)},
            device_id_type=MESH,
        )

    def cross_copy(d, p, i, owner, recv_sem):
        piece = attended_part(owner, d, p, i)
        return pltpu.make_async_remote_copy(
            src_ref=piece, dst_ref=piece, send_sem=la_send,
            recv_sem=recv_sem, device_id=partner, device_id_type=MESH,
        )

    def cross_over(d, p, i):
        @pl.when(p < pairs - 1)
        def _():
            cross_copy(d, p, i, col, lp_recv.at[jnp.minimum(p, pairs - 2)]).start()

        @pl.when(p == pairs - 1)
        def _():
            cross_copy(d, p, i, col, la_recv.at[d, i]).start()

    def attend_piece(d, p, i):
        rows = pl.ds(pl.multiple_of(i * PIECE, PIECE), PIECE)
        first = (col * 2 + d) * WIDE
        for h in range(2):
            at = slice(h * K, (h + 1) * K)
            k = summed[d, 3 * p, :, at]
            v = summed[d, 3 * p + 1, :, at]
            q = summed[d, 3 * p + 2, rows, at]
            scores = lax.dot_general(
                q, k, (((1,), (1,)), ((), ())), preferred_element_type=f32
            )
            exponent = jnp.exp2(
                (scores - jnp.max(scores, axis=1, keepdims=True)) * (scaling * math.log2(math.e))
            )
            mixed = jnp.dot(exponent.astype(bf16), v, preferred_element_type=f32)
            attended[p, rows, pl.ds(pl.multiple_of(first + h * K, K), K)] = (
                mixed / jnp.sum(exponent, axis=1, keepdims=True)
            ).astype(bf16)

    def spread_statistics():
        for o in range(1, rows_n):
            stat_copy(0, lax.rem(z + o, rows_n)).wait_recv()
        mean = sum(stats[i, 0] for i in range(rows_n)) * (1.0 / rows_n)
        spread = sum(
            stats[i, 1] * (1.0 / block) + (stats[i, 0] - mean) * (stats[i, 0] - mean)
            for i in range(rows_n)
        ) * (1.0 / rows_n)
        scale = lax.rsqrt(spread + EPSILON)
        for i in range(rows_n):
            shift = (stats[i, 0] - mean) * scale
            spread_col[i] = jnp.broadcast_to(shift, (128, tokens_n)).T
        spread_col[rows_n] = jnp.broadcast_to(scale, (128, tokens_n)).T

    def weights_ready(p):
        rows = late_w.at[p, pl.ds(0, 2 * WIDE)]
        pltpu.make_async_copy(rows, rows, late_sem.at[p]).wait()
        for recvs in (lc_recv, ld_recv):
            landed(late_w.at[p, pl.ds(0, 2 * quarter)], recvs.at[p])

    def pair_ready(p):
        weights_ready(p)
        landed(summed.at[0, pl.ds(0, 2)], lp_recv.at[p])

    def fold(p, rows, at):
        return jnp.dot(attended[p, rows, :], late_w[p, :, at], preferred_element_type=f32)

    nearer = jnp.where(z < last_place - z, 1, 0)
    starts = (z == 0) | (z == last_place)

    def centre(i):
        tok_copy(i).wait()

        @pl.loop(0, PIECE // ROWS)
        def _(j):
            at = pl.ds(pl.multiple_of(i * PIECE + j * ROWS, ROWS), ROWS)
            x = tok[at, :].astype(f32)
            mean = jnp.sum(x, axis=1, keepdims=True) * (1.0 / block)
            away = x - mean
            square = jnp.sum(away * away, axis=1, keepdims=True)
            normed[at, :] = (away * gain_row[...]).astype(bf16)
            stat_col[0, at, :] = jnp.broadcast_to(mean, (ROWS, 128))
            stat_col[1, at, :] = jnp.broadcast_to(square, (ROWS, 128))

    def first_piece(i):
        rows = pl.ds(pl.multiple_of(i * PIECE, PIECE), PIECE)
        summed[nearer, 0, rows] = jnp.dot(
            normed[rows, :], wide_w[nearer, 0], preferred_element_type=f32
        ).astype(bf16)

    centre(0)

    @pl.when(starts)
    def _():
        weight_copy(nearer, 0).wait()
        first_piece(0)

    pl.semaphore_wait(barrier, rows_n + 2)

    @pl.when(starts)
    def _():
        sum_copy(nearer, 0, 0).start()


    @pl.loop(1, pieces)
    def _(i):
        centre(i)

        @pl.when(starts)
        def _():
            first_piece(i)
            sum_copy(nearer, 0, i).start()

    @pl.when(starts)
    def _():
        value = jnp.dot(
            normed[pl.ds(tokens_n, EXTRA), :], wide_w[nearer, 0], preferred_element_type=f32
        )
        gain_sum[nearer, 0] = value[0:1] + value[1:2]
        gain_copy(nearer, 0, z).start()

    def offset(pos):
        return jnp.where(pos > 0, LEAD + SKEW * pos, -pieces)

    end_offset = LEAD + SKEW * last_place
    blocks = stream_blocks(pairs, pieces, end_offset + pieces + 1)
    slots = blocks[-1][3] + pieces + end_offset
    every = pl.ds(0, tokens_n)

    def fold_pair(p):
        pair_ready(p)
        for j in range(tiles // 2):
            at = slice(j * 2 * WIDE, (j + 1) * 2 * WIDE)
            value = fold(p, every, at)
            total[:, at] = value if p == 0 else total[:, at] + value

    stat_slot = jnp.where(starts, 0, LEAD + SKEW + 1)

    def multiply(d, c, pos):
        weight_copy(d, c).wait()
        value = jnp.dot(normed[...], wide_w[d, c], preferred_element_type=f32)
        part[d, c % 2] = value[0:tokens_n]
        gain_value = value[tokens_n:tokens_n + 1] + value[tokens_n + 1:tokens_n + 2]

        @pl.when(pos < last_place)
        def _():
            gain_sum[d, c] = gain_value
            gain_copy(d, c, z).start()

        @pl.when(pos == last_place)
        def _():
            gain_all[c, z] = gain_value

    @pl.when(starts)
    def _():
        multiply(nearer, 1, 0)

    @pl.loop(0, slots)
    def _(t):
        @pl.when(t == stat_slot + 1)
        def _():
            @pl.loop(0, pairs)
            def _(p):
                share_copy(0, p, col).start()
                share_copy(1, p, col).start()

        @pl.when(t == stat_slot)
        def _():
            stats[z, 0] = stat_col[0].T[0:1]
            stats[z, 1] = stat_col[1].T[0:1]
            for which in range(2):
                @pl.when(z != which * last_place)
                def _():
                    stat_copy(which, z).start()

        @pl.when((t == end_offset - 1) & starts)
        def _():
            spread_statistics()

        ahead = []
        for k in range(2):
            d = nearer if k == 0 else 1 - nearer
            pos = place(d)
            n = t - offset(pos)
            u = n
            returns = False
            back_pair, back_piece = 0, 0
            for p, piece, count, begin in blocks:
                inside = (n >= begin) & (n < begin + count)
                returns = returns | inside
                back_pair = jnp.where(inside, p, back_pair)
                back_piece = jnp.where(inside, n - begin + piece, back_piece)
                u = jnp.where(n >= begin + count, u - count, u)
            c, i = u // pieces, u % pieces

            @pl.when((u >= 0) & (u < units) & jnp.logical_not(returns))
            def _():
                rows = pl.ds(pl.multiple_of(i * PIECE, PIECE), PIECE)

                side = c % 2

                @pl.when((i == 0) & (pos == last_place))
                def _():
                    landed(gain_all.at[c, pl.ds(0, last_place)], gs_recv.at[c])

                @pl.when(pos == 0)
                def _():
                    summed[d, c, rows] = part[d, side, rows].astype(bf16)

                @pl.when(pos > 0)
                def _():
                    sum_copy(d, c, i).wait_recv()

                @pl.when((pos > 0) & (pos < last_place))
                def _():
                    summed[d, c, rows] = (part[d, side, rows] + arrived[d, c, rows].astype(f32)).astype(bf16)

                @pl.when(pos < last_place)
                def _():
                    sum_copy(d, c, i).start()

                @pl.when(pos == last_place)
                def _():
                    scale = spread_col[rows_n, rows]
                    for h in range(2):
                        lanes = slice(h * 128, (h + 1) * 128)
                        whole = part[d, side, rows, lanes] + arrived[d, c, rows, lanes].astype(f32)
                        whole = whole * scale
                        for source in range(rows_n):
                            whole = whole + spread_col[source, rows] * gain_all[c, source, :, lanes]
                        summed[d, c, rows, lanes] = whole.astype(bf16)

                @pl.when((pos == last_place) & (c % 3 == 2))
                def _():
                    attend_piece(d, c // 3, i)
                    cross_over(d, c // 3, i)

            ahead.append(
                (d, pos, u + 1, (u >= -1) & (u < units - 1) & jnp.logical_not(returns))
            )

            @pl.when(returns)
            def _():
                p, other = back_pair, 1 - d
                turned = (p == pairs - 1) & (pos == last_place)
                s = jnp.where(turned, (back_piece + pieces - DIRECT) % pieces, back_piece)
                direct = (p == pairs - 1) & (s >= pieces - DIRECT)

                @pl.when(pos > 0)
                def _():
                    attended_copy(other, p, s).wait_recv()

                @pl.when((pos < last_place) & jnp.logical_not(direct))
                def _():
                    attended_copy(other, p, s).start()

                @pl.when((pos == 0) & direct)
                def _():
                    for o in range(last_place, 0, -1):
                        direct_copy(other, p, s, o).start()

                @pl.when(pos > 0)
                def _():
                    cross_over(other, p, s)

        for d, pos, u, due in ahead:
            @pl.when(due & (u % pieces == 0))
            def _():
                multiply(d, u // pieces, pos)

        @pl.when((t >= HAND) & (t < HAND + 2 * pieces * pairs) & ((t - HAND) % (2 * pieces) == 0))
        def _():
            p = (t - HAND) // (2 * pieces)
            landed(late_w.at[p, pl.ds(0, 2 * quarter)], lx_recv.at[p])
            for d in range(2):
                across_copy(d, p, dp).start()
                near_copy(d, p, dp).start()

        @pl.when(
            (t >= HAND_ON) & (t < HAND_ON + 2 * pieces * pairs)
            & ((t - HAND_ON) % (2 * pieces) == 0)
        )
        def _():
            p = (t - HAND_ON) // (2 * pieces)
            landed(late_w.at[p, pl.ds(0, 2 * quarter)], ly_recv.at[p])
            for d in range(2):
                far_copy(d, p, across_at).start()

        @pl.when(t == blocks[-2][3] + blocks[-2][2] + end_offset)
        def _():
            for p in range(pairs - 2):
                fold_pair(p)

    final = pairs - 1
    fold_pair(final - 1)
    weights_ready(final)

    def fold_owner(rows, at, owner):
        heads = pl.ds(pl.multiple_of(owner * 2 * WIDE, 2 * WIDE), 2 * WIDE)
        return jnp.dot(
            attended[final, rows, heads], late_w[final, heads, at], preferred_element_type=f32
        )

    for j in range(tiles // 2):
        at = slice(j * 2 * WIDE, (j + 1) * 2 * WIDE)
        total[:, at] = total[:, at] + fold_owner(every, at, col)

    for first in range(0, pieces, GROUP):
        group = range(first, min(first + GROUP, pieces))
        rows = slice(first * PIECE, (group[-1] + 1) * PIECE)
        for d in range(2):
            for i in group:
                cross_copy(d, final, i, 1 - col, la_recv.at[d, i]).wait_recv()
        for j in range(tiles // 2):
            at = slice(j * 2 * WIDE, (j + 1) * 2 * WIDE)
            out[rows, at] = (total[rows, at] + fold_owner(rows, at, 1 - col)).astype(bf16)

    for which in range(2):
        @pl.when(z != which * last_place)
        def _():
            stat_copy(which, z).wait_send()
    for d in range(2):
        pos = place(d)

        @pl.when(pos < last_place)
        def _():
            sent(gain_sum.at[d], gs_send.at[d])
            sent(summed.at[d], rs_send.at[d])

        @pl.when(pos > 0)
        def _():
            sent(wide_w.at[0, 0, pl.ds(0, pairs * tokens_n - DIRECT * PIECE)], at_send.at[d])

        @pl.when(pos == last_place)
        def _():
            sent(wide_w.at[0, 0, pl.ds(0, last_place * DIRECT * PIECE)], di_send)

    sent(summed.at[0, pl.ds(0, 2 * pairs)], la_send)
    for sem in (lx_send, ly_send, lc_send, ld_send):
        sent(late_w.at[0, pl.ds(0, 2 * pairs * quarter)], sem)


def fused_shards(rows_n, dp_n, tokens, norm_gain, qkv_weight, out_weight):
    tokens_n, block = tokens.shape
    pairs = qkv_weight.shape[2] // (2 * WIDE)
    chunks = 3 * pairs
    pieces = tokens_n // PIECE
    any_space = pl.BlockSpec(memory_space=pl.ANY)
    vmem = pl.BlockSpec(memory_space=pltpu.VMEM)
    hbm = pl.BlockSpec(memory_space=pltpu.HBM)
    dma = pltpu.SemaphoreType.DMA
    bf16, f32 = jnp.bfloat16, jnp.float32
    return pl.pallas_call(
        functools.partial(sublayer_kernel, rows_n, dp_n),
        out_shape=pltpu.VMEM((tokens_n, block), bf16),
        in_specs=[any_space, hbm, any_space, any_space],
        out_specs=vmem,
        scratch_shapes=[
            pltpu.VMEM((tokens_n, block), bf16),
            pltpu.VMEM((2, chunks, block, WIDE), bf16),
            pltpu.VMEM((block // 128, 128), f32),
            pltpu.VMEM((1, block), f32),
            pltpu.VMEM((2, tokens_n, 128), f32),
            pltpu.VMEM((rows_n, 2, 1, tokens_n), f32),
            pltpu.VMEM((rows_n + 1, tokens_n, 128), f32),
            pltpu.VMEM((tokens_n + EXTRA, block), bf16),
            pltpu.VMEM((2, 2, tokens_n, WIDE), f32),
            pltpu.VMEM((2, chunks, 1, WIDE), f32),
            pltpu.VMEM((chunks, rows_n, 1, WIDE), f32),
            pltpu.VMEM((2, chunks, tokens_n, WIDE), bf16),
            pltpu.VMEM((2, chunks, tokens_n, WIDE), bf16),
            pltpu.VMEM((pairs, tokens_n, 4 * WIDE), bf16),
            pltpu.VMEM((pairs, 4 * WIDE, block), bf16),
            pltpu.VMEM((tokens_n, block), f32),
            dma((pieces,)), dma, dma((2, chunks)), dma((pairs,)),
            dma((2,)), dma((rows_n,)), dma((2,)), dma((chunks,)),
            dma((2,)), dma((2, chunks, pieces)),
            dma((2,)), dma((2, pairs, pieces)), dma, dma((pairs - 1,)),
            dma, dma((2, pieces)), dma, dma((pairs,)), dma, dma((pairs,)),
            dma, dma((pairs,)), dma, dma((pairs,)),
        ],
        compiler_params=pltpu.CompilerParams(
            collective_id=0, has_side_effects=True, vmem_limit_bytes=65800000
        ),
    )(
        tokens, norm_gain.reshape(block // 128, 128), jnp.transpose(qkv_weight, (1, 0, 2)),
        out_weight,
    )


def solution(mesh):
    in_specs = (P("dp", "row"), P("row"), P("row", None, "col"), P("col", "row"))
    out_specs = P("dp", "row")
    rows_n, cols_n, dp_n = mesh.shape["row"], mesh.shape["col"], mesh.shape["dp"]

    def body(tokens, norm_gain, qkv_weight, out_weight):
        tokens_n, block = tokens.shape
        fits = (
            cols_n == 2 and dp_n == 4 and rows_n >= 2 and qkv_weight.shape[2] % (2 * WIDE) == 0
            and qkv_weight.shape[2] >= 4 * WIDE
            and block % (2 * WIDE) == 0 and tokens_n % PIECE == 0
            and (qkv_weight.shape[2] // (2 * WIDE)) * tokens_n <= block
            and (rows_n - 1) * DIRECT * PIECE <= block and tokens_n > DIRECT * PIECE
        )
        if fits:
            return fused_shards(rows_n, dp_n, tokens, norm_gain, qkv_weight, out_weight)
        return shards(tokens, norm_gain, qkv_weight, out_weight)

    return jax.shard_map(body, mesh=mesh, in_specs=in_specs, out_specs=out_specs, check_vma=False)
```

```python
import functools
import math

import jax
import jax.numpy as jnp
from jax import lax
from jax.experimental import pallas as pl
from jax.experimental.pallas import tpu as pltpu
from jax.sharding import PartitionSpec as P

K = 128


EPSILON = 1e-05


def attend(queries, key_rows, value_rows):
    query_total = queries.shape[0]
    head_count = queries.shape[1] // K
    scaling = 1.0 / math.sqrt(K)
    split_keys = key_rows.reshape(key_rows.shape[0], head_count, K)
    split_values = value_rows.reshape(value_rows.shape[0], head_count, K)
    split_queries = queries.reshape(query_total, head_count, K)
    scores = (
        jnp.einsum("qhd,khd->hqk", split_queries, split_keys, preferred_element_type=jnp.float32)
        * scaling
    )
    largest = jnp.max(scores, axis=2, keepdims=True)
    exponent = jnp.exp(scores - largest)
    softmax_weights = (exponent / jnp.sum(exponent, axis=2, keepdims=True)).astype(jnp.bfloat16)
    mixed = jnp.einsum(
        "hqk,khd->qhd", softmax_weights, split_values, preferred_element_type=jnp.float32
    )
    result = mixed.astype(jnp.bfloat16)
    return result.reshape(query_total, head_count * K)


def shards(tokens, norm_gain, qkv_weight, out_weight):
    row_count, block_width = tokens.shape
    full_width = block_width * lax.axis_size("row")
    values = tokens.astype(jnp.float32)
    totals, squares = lax.psum(
        (jnp.sum(values, axis=1, keepdims=True), jnp.sum(values * values, axis=1, keepdims=True)),
        "row",
    )
    average = totals / full_width
    variance = squares / full_width - average * average
    centered = values - average
    normed = (centered * lax.rsqrt(variance + EPSILON) * norm_gain).astype(jnp.bfloat16)
    head_columns = qkv_weight.shape[2]
    partial_value = jnp.dot(
        normed,
        qkv_weight.reshape(block_width, 3 * head_columns),
        preferred_element_type=jnp.float32,
    )
    summed = lax.psum(partial_value.astype(jnp.bfloat16), "row").reshape(row_count, 3, head_columns)
    attended = attend(summed[:, 0], summed[:, 1], summed[:, 2])
    partial_out = jnp.dot(attended, out_weight, preferred_element_type=jnp.float32)
    return lax.psum(partial_out.astype(jnp.bfloat16), "col")


MESH = pl.DeviceIdType.MESH
WIDE = 2 * K
ROWS = 32
EXTRA = 16
PIECE = 96
GROUP = 2
DIRECT = 1
EARLY = 3
SKEW = 3
LEAD = 1
HAND = 18
HAND_ON = 32


def stream_blocks(pairs, pieces, lag):
    place, unit, blocks, asked = 0, 0, [], {}
    early = min(EARLY, pieces)
    while unit < 3 * pairs * pieces:
        following = len(blocks)
        if early and following < pairs - 2 and place >= asked.get(following, place + 1) + lag:
            blocks.append((following, 0, early, place))
            place += early
            continue
        if unit % (3 * pieces) == 2 * pieces:
            asked[unit // (3 * pieces)] = place
        unit += 1
        place += 1
    gone = len(blocks)
    for pair in range(pairs):
        first = early if pair < gone else 0
        if first < pieces:
            place = max(place, asked[pair] + first + lag)
            blocks.append((pair, first, pieces - first, place))
            place += pieces - first
    return blocks


def sublayer_kernel(
    rows_n, dp_n, tok_hbm, gain_hbm, w_hbm, wo_hbm, out,
    tok, wide_w, gain_ref, gain_row, stat_col, stats, spread_col, normed, part, gain_sum, gain_all,
    arrived, summed, attended, late_w, total,
    tok_sem, gain_sem, w_sem, late_sem, st_send, st_recv, gs_send, gs_recv, rs_send, rs_recv,
    at_send, at_recv, ah_recv, di_send, lp_recv, la_send, la_recv, lx_send, lx_recv, ly_send, ly_recv, lc_send, lc_recv,
    ld_send, ld_recv,
):
    z = lax.axis_index("row")
    col = lax.axis_index("col")
    dp = lax.axis_index("dp")
    tokens_n, block = tok.shape
    half = w_hbm.shape[2] // 2
    pairs = half // WIDE
    chunks = 3 * pairs
    pieces = tokens_n // PIECE
    units = chunks * pieces
    tiles = block // WIDE
    quarter = WIDE // dp_n
    partner = {"col": 1 - col}
    sibling_at = dp + 1 - 2 * (dp % 2)
    across_at = (dp + 2) % dp_n
    sibling, across = {"dp": sibling_at}, {"dp": across_at}
    scaling = 1.0 / math.sqrt(K)
    last_place = rows_n - 1
    f32, bf16 = jnp.float32, jnp.bfloat16

    def weight_copy(d, c):
        pair, kind = c // 3, (c + 1) % 3
        first = pl.multiple_of(d * half + pair * WIDE, WIDE)
        return pltpu.make_async_copy(
            w_hbm.at[kind, :, pl.ds(first, WIDE)], wide_w.at[d, c], w_sem.at[d, c]
        )

    gain_load = pltpu.make_async_copy(gain_hbm, gain_ref, gain_sem)
    gain_load.start()

    def tok_copy(i):
        rows = pl.ds(pl.multiple_of(i * PIECE, PIECE), PIECE)
        return pltpu.make_async_copy(tok_hbm.at[rows], tok.at[rows], tok_sem.at[i])

    @pl.loop(0, pieces)
    def _(i):
        tok_copy(i).start()

    early_side = jnp.where(2 * z < rows_n - 1, 1, 0)
    for c in range(2):
        weight_copy(early_side, c).start()
    for c in range(2):
        weight_copy(1 - early_side, c).start()

    @pl.loop(2, chunks)
    def _(c):
        weight_copy(0, c).start()
        weight_copy(1, c).start()

    def head_columns(owner, d):
        return pl.ds(pl.multiple_of((owner * 2 + d) * WIDE, WIDE), WIDE)

    def own_copy(d, p):
        rows = pl.ds(d * half + p * WIDE, WIDE)
        return pltpu.make_async_copy(
            wo_hbm.at[rows], late_w.at[p, head_columns(col, d)], late_sem.at[p]
        )

    def quarter_at(owner, d, which):
        first = (owner * 2 + d) * WIDE + which * quarter
        return pl.ds(pl.multiple_of(first, quarter), quarter)

    def share_copy(d, p, owner):
        first = pl.multiple_of(d * half + p * WIDE + dp * quarter, quarter)
        return pltpu.make_async_remote_copy(
            src_ref=wo_hbm.at[pl.ds(first, quarter)],
            dst_ref=late_w.at[p, quarter_at(owner, d, dp)],
            send_sem=lx_send, recv_sem=lx_recv.at[p], device_id=partner,
            device_id_type=MESH,
        )

    def pass_copy(d, p, which, sends, recvs, device):
        piece = late_w.at[p, quarter_at(1 - col, d, which)]
        return pltpu.make_async_remote_copy(
            src_ref=piece, dst_ref=piece, send_sem=sends, recv_sem=recvs.at[p],
            device_id=device, device_id_type=MESH,
        )

    def across_copy(d, p, which):
        return pass_copy(d, p, which, ly_send, ly_recv, across)

    def near_copy(d, p, which):
        return pass_copy(d, p, which, lc_send, lc_recv, sibling)

    def far_copy(d, p, which):
        return pass_copy(d, p, which, ld_send, ld_recv, sibling)

    def whole(source, sem):
        return pltpu.make_async_remote_copy(
            src_ref=source, dst_ref=source, send_sem=sem, recv_sem=sem,
            device_id=partner, device_id_type=MESH,
        )

    def sent(source, sem):
        whole(source, sem).wait_send()

    def landed(target, sem):
        whole(target, sem).wait_recv()

    @pl.loop(0, pairs)
    def _(p):
        own_copy(0, p).start()
        own_copy(1, p).start()

    barrier = pltpu.get_barrier_semaphore()
    for o in range(1, rows_n):
        pl.semaphore_signal(
            barrier, inc=1, device_id={"row": lax.rem(z + o, rows_n)}, device_id_type=MESH
        )
    for device in (partner, sibling, across):
        pl.semaphore_signal(barrier, inc=1, device_id=device, device_id_type=MESH)

    gain_load.wait()
    for j in range(block // 128):
        gain_row[0:1, j * 128:(j + 1) * 128] = gain_ref[j:j + 1, :]
    gain = gain_row[...]
    high = gain.astype(bf16).astype(f32)
    row = lax.broadcasted_iota(jnp.int32, (EXTRA, block), 0)
    normed[pl.ds(tokens_n, EXTRA), :] = jnp.where(
        row == 0, high, jnp.where(row == 1, gain - high, 0.0)
    ).astype(bf16)
    def place(d):
        return jnp.where(d == 1, z, last_place - z)

    def end_of(d):
        return jnp.where(d == 1, last_place, 0)

    def onward(d):
        return {"row": jnp.clip(jnp.where(d == 1, z + 1, z - 1), 0, last_place)}

    def back(d):
        return {"row": jnp.clip(jnp.where(d == 1, z - 1, z + 1), 0, last_place)}

    def stat_copy(which, source):
        return pltpu.make_async_remote_copy(
            src_ref=stats.at[source], dst_ref=stats.at[source], send_sem=st_send.at[which],
            recv_sem=st_recv.at[source], device_id={"row": which * last_place},
            device_id_type=MESH,
        )

    def gain_copy(d, c, source):
        return pltpu.make_async_remote_copy(
            src_ref=gain_sum.at[d, c], dst_ref=gain_all.at[c, source], send_sem=gs_send.at[d],
            recv_sem=gs_recv.at[c], device_id={"row": end_of(d)}, device_id_type=MESH,
        )

    def sum_copy(d, c, i):
        at = pl.ds(pl.multiple_of(i * PIECE, PIECE), PIECE)
        return pltpu.make_async_remote_copy(
            src_ref=summed.at[d, c, at], dst_ref=arrived.at[d, c, at],
            send_sem=rs_send.at[d], recv_sem=rs_recv.at[d, (c * pieces + i) % rs_recv.shape[1]],
            device_id=onward(d), device_id_type=MESH,
        )

    def attended_part(owner, d, p, i):
        rows = pl.ds(pl.multiple_of(i * PIECE, PIECE), PIECE)
        return attended.at[p, rows, head_columns(owner, d)]

    def attended_copy(d, p, i):
        piece = attended_part(col, d, p, i)
        return pltpu.make_async_remote_copy(
            src_ref=piece, dst_ref=piece, send_sem=at_send.at[d],
            recv_sem=at_recv.at[d, p, i], device_id=back(d), device_id_type=MESH,
        )

    def half_part(owner, d, i, h):
        first = pl.multiple_of(i * PIECE + h * (PIECE // 2), PIECE // 2)
        return attended.at[pairs - 1, pl.ds(first, PIECE // 2), head_columns(owner, d)]

    def half_copy(d, i, h):
        piece = half_part(col, d, i, h)
        return pltpu.make_async_remote_copy(
            src_ref=piece, dst_ref=piece, send_sem=at_send.at[d],
            recv_sem=ah_recv.at[d, i, h], device_id=back(d), device_id_type=MESH,
        )

    def half_cross(d, i, h):
        piece = half_part(col, d, i, h)
        return pltpu.make_async_remote_copy(
            src_ref=piece, dst_ref=piece, send_sem=la_send,
            recv_sem=la_recv.at[d, i], device_id=partner, device_id_type=MESH,
        )

    def direct_copy(d, p, i, o):
        piece = attended_part(col, d, p, i)
        return pltpu.make_async_remote_copy(
            src_ref=piece, dst_ref=piece, send_sem=di_send,
            recv_sem=at_recv.at[d, p, i],
            device_id={"row": jnp.clip(jnp.where(d == 1, z - o, z + o), 0, last_place)},
            device_id_type=MESH,
        )

    def cross_copy(d, p, i, owner, recv_sem):
        piece = attended_part(owner, d, p, i)
        return pltpu.make_async_remote_copy(
            src_ref=piece, dst_ref=piece, send_sem=la_send,
            recv_sem=recv_sem, device_id=partner, device_id_type=MESH,
        )

    def cross_over(d, p, i):
        @pl.when(p < pairs - 1)
        def _():
            cross_copy(d, p, i, col, lp_recv.at[jnp.minimum(p, pairs - 2)]).start()

        @pl.when(p == pairs - 1)
        def _():
            cross_copy(d, p, i, col, la_recv.at[d, i]).start()

    def attend_piece(d, p, i):
        rows = pl.ds(pl.multiple_of(i * PIECE, PIECE), PIECE)
        first = (col * 2 + d) * WIDE
        for h in range(2):
            at = slice(h * K, (h + 1) * K)
            k = summed[d, 3 * p, :, at]
            v = summed[d, 3 * p + 1, :, at]
            q = summed[d, 3 * p + 2, rows, at]
            scores = lax.dot_general(
                q, k, (((1,), (1,)), ((), ())), preferred_element_type=f32
            )
            exponent = jnp.exp2(
                (scores - jnp.max(scores, axis=1, keepdims=True)) * (scaling * math.log2(math.e))
            )
            mixed = jnp.dot(exponent.astype(bf16), v, preferred_element_type=f32)
            attended[p, rows, pl.ds(pl.multiple_of(first + h * K, K), K)] = (
                mixed / jnp.sum(exponent, axis=1, keepdims=True)
            ).astype(bf16)

    def spread_statistics():
        for o in range(1, rows_n):
            stat_copy(0, lax.rem(z + o, rows_n)).wait_recv()
        mean = sum(stats[i, 0] for i in range(rows_n)) * (1.0 / rows_n)
        spread = sum(
            stats[i, 1] * (1.0 / block) + (stats[i, 0] - mean) * (stats[i, 0] - mean)
            for i in range(rows_n)
        ) * (1.0 / rows_n)
        scale = lax.rsqrt(spread + EPSILON)
        for i in range(rows_n):
            shift = (stats[i, 0] - mean) * scale
            spread_col[i] = jnp.broadcast_to(shift, (128, tokens_n)).T
        spread_col[rows_n] = jnp.broadcast_to(scale, (128, tokens_n)).T

    def weights_ready(p):
        rows = late_w.at[p, pl.ds(0, 2 * WIDE)]
        pltpu.make_async_copy(rows, rows, late_sem.at[p]).wait()
        for recvs in (lc_recv, ld_recv):
            landed(late_w.at[p, pl.ds(0, 2 * quarter)], recvs.at[p])

    def pair_ready(p):
        weights_ready(p)
        landed(summed.at[0, pl.ds(0, 2)], lp_recv.at[p])

    def fold(p, rows, at):
        return jnp.dot(attended[p, rows, :], late_w[p, :, at], preferred_element_type=f32)

    nearer = jnp.where(z < last_place - z, 1, 0)
    starts = (z == 0) | (z == last_place)

    def centre(i):
        tok_copy(i).wait()

        @pl.loop(0, PIECE // ROWS)
        def _(j):
            at = pl.ds(pl.multiple_of(i * PIECE + j * ROWS, ROWS), ROWS)
            x = tok[at, :].astype(f32)
            mean = jnp.sum(x, axis=1, keepdims=True) * (1.0 / block)
            away = x - mean
            square = jnp.sum(away * away, axis=1, keepdims=True)
            normed[at, :] = (away * gain_row[...]).astype(bf16)
            stat_col[0, at, :] = jnp.broadcast_to(mean, (ROWS, 128))
            stat_col[1, at, :] = jnp.broadcast_to(square, (ROWS, 128))

    def first_piece(i):
        rows = pl.ds(pl.multiple_of(i * PIECE, PIECE), PIECE)
        summed[nearer, 0, rows] = jnp.dot(
            normed[rows, :], wide_w[nearer, 0], preferred_element_type=f32
        ).astype(bf16)

    centre(0)

    @pl.when(starts)
    def _():
        weight_copy(nearer, 0).wait()
        first_piece(0)

    pl.semaphore_wait(barrier, rows_n + 2)

    @pl.when(starts)
    def _():
        sum_copy(nearer, 0, 0).start()


    @pl.loop(1, pieces)
    def _(i):
        centre(i)

        @pl.when(starts)
        def _():
            first_piece(i)
            sum_copy(nearer, 0, i).start()

    @pl.when(starts)
    def _():
        value = jnp.dot(
            normed[pl.ds(tokens_n, EXTRA), :], wide_w[nearer, 0], preferred_element_type=f32
        )
        gain_sum[nearer, 0] = value[0:1] + value[1:2]
        gain_copy(nearer, 0, z).start()

    def offset(pos):
        return jnp.where(pos > 0, LEAD + SKEW * pos, -pieces)

    end_offset = LEAD + SKEW * last_place
    blocks = stream_blocks(pairs, pieces, end_offset + pieces + 1)
    slots = blocks[-1][3] + pieces + end_offset
    every = pl.ds(0, tokens_n)

    def fold_pair(p):
        pair_ready(p)
        for j in range(tiles // 2):
            at = slice(j * 2 * WIDE, (j + 1) * 2 * WIDE)
            value = fold(p, every, at)
            total[:, at] = value if p == 0 else total[:, at] + value

    stat_slot = jnp.where(starts, 0, LEAD + SKEW + 1)

    def multiply(d, c, pos):
        weight_copy(d, c).wait()
        value = jnp.dot(normed[...], wide_w[d, c], preferred_element_type=f32)
        part[d, c % 2] = value[0:tokens_n]
        gain_value = value[tokens_n:tokens_n + 1] + value[tokens_n + 1:tokens_n + 2]

        @pl.when(pos < last_place)
        def _():
            gain_sum[d, c] = gain_value
            gain_copy(d, c, z).start()

        @pl.when(pos == last_place)
        def _():
            gain_all[c, z] = gain_value

    @pl.when(starts)
    def _():
        multiply(nearer, 1, 0)

    @pl.loop(0, slots)
    def _(t):
        @pl.when(t == stat_slot + 4)
        def _():
            @pl.loop(0, pairs)
            def _(p):
                share_copy(0, p, col).start()
                share_copy(1, p, col).start()

        @pl.when(t == stat_slot)
        def _():
            stats[z, 0] = stat_col[0].T[0:1]
            stats[z, 1] = stat_col[1].T[0:1]
            for which in range(2):
                @pl.when(z != which * last_place)
                def _():
                    stat_copy(which, z).start()

        @pl.when((t == end_offset - 1) & starts)
        def _():
            spread_statistics()

        ahead = []
        for k in range(2):
            d = nearer if k == 0 else 1 - nearer
            pos = place(d)
            n = t - offset(pos)
            u = n
            returns = False
            back_pair, back_piece = 0, 0
            for p, piece, count, begin in blocks:
                inside = (n >= begin) & (n < begin + count)
                returns = returns | inside
                back_pair = jnp.where(inside, p, back_pair)
                back_piece = jnp.where(inside, n - begin + piece, back_piece)
                u = jnp.where(n >= begin + count, u - count, u)
            c, i = u // pieces, u % pieces

            @pl.when((u >= 0) & (u < units) & jnp.logical_not(returns))
            def _():
                rows = pl.ds(pl.multiple_of(i * PIECE, PIECE), PIECE)

                side = c % 2

                @pl.when((i == 0) & (pos == last_place))
                def _():
                    landed(gain_all.at[c, pl.ds(0, last_place)], gs_recv.at[c])

                @pl.when(pos == 0)
                def _():
                    summed[d, c, rows] = part[d, side, rows].astype(bf16)

                @pl.when(pos > 0)
                def _():
                    sum_copy(d, c, i).wait_recv()

                @pl.when((pos > 0) & (pos < last_place))
                def _():
                    summed[d, c, rows] = (part[d, side, rows] + arrived[d, c, rows].astype(f32)).astype(bf16)

                @pl.when(pos < last_place)
                def _():
                    sum_copy(d, c, i).start()

                @pl.when(pos == last_place)
                def _():
                    scale = spread_col[rows_n, rows]
                    for h in range(2):
                        lanes = slice(h * 128, (h + 1) * 128)
                        whole = part[d, side, rows, lanes] + arrived[d, c, rows, lanes].astype(f32)
                        whole = whole * scale
                        for source in range(rows_n):
                            whole = whole + spread_col[source, rows] * gain_all[c, source, :, lanes]
                        summed[d, c, rows, lanes] = whole.astype(bf16)

                @pl.when((pos == last_place) & (c % 3 == 2))
                def _():
                    attend_piece(d, c // 3, i)
                    cross_over(d, c // 3, i)

            ahead.append(
                (d, pos, u + 1, (u >= -1) & (u < units - 1) & jnp.logical_not(returns))
            )

            @pl.when(returns)
            def _():
                p, other = back_pair, 1 - d
                turned = (p == pairs - 1) & (pos == last_place)
                s = jnp.where(turned, (back_piece + pieces - DIRECT) % pieces, back_piece)
                direct = (p == pairs - 1) & (s >= pieces - DIRECT)

                halved = (p == pairs - 1) & jnp.logical_not(direct)

                @pl.when(halved)
                def _():
                    for h in range(2):
                        @pl.when(pos > 0)
                        def _():
                            half_copy(other, s, h).wait_recv()

                        @pl.when(pos < last_place)
                        def _():
                            half_copy(other, s, h).start()

                        @pl.when(pos > 0)
                        def _():
                            half_cross(other, s, h).start()

                @pl.when(jnp.logical_not(halved) & (pos > 0))
                def _():
                    attended_copy(other, p, s).wait_recv()

                @pl.when((pos < last_place) & jnp.logical_not(halved | direct))
                def _():
                    attended_copy(other, p, s).start()

                @pl.when((pos == 0) & direct)
                def _():
                    for o in range(last_place, 0, -1):
                        direct_copy(other, p, s, o).start()

                @pl.when(jnp.logical_not(halved) & (pos > 0))
                def _():
                    cross_over(other, p, s)

        for d, pos, u, due in ahead:
            @pl.when(due & (u % pieces == 0))
            def _():
                multiply(d, u // pieces, pos)

        @pl.when((t >= HAND) & (t < HAND + 2 * pieces * pairs) & ((t - HAND) % (2 * pieces) == 0))
        def _():
            p = (t - HAND) // (2 * pieces)
            landed(late_w.at[p, pl.ds(0, 2 * quarter)], lx_recv.at[p])
            for d in range(2):
                across_copy(d, p, dp).start()
                near_copy(d, p, dp).start()

        @pl.when(
            (t >= HAND_ON) & (t < HAND_ON + 2 * pieces * pairs)
            & ((t - HAND_ON) % (2 * pieces) == 0)
        )
        def _():
            p = (t - HAND_ON) // (2 * pieces)
            landed(late_w.at[p, pl.ds(0, 2 * quarter)], ly_recv.at[p])
            for d in range(2):
                far_copy(d, p, across_at).start()

        @pl.when(t == blocks[-2][3] + blocks[-2][2] + end_offset)
        def _():
            for p in range(pairs - 2):
                fold_pair(p)

    final = pairs - 1
    fold_pair(final - 1)
    weights_ready(final)

    def fold_owner(rows, at, owner):
        heads = pl.ds(pl.multiple_of(owner * 2 * WIDE, 2 * WIDE), 2 * WIDE)
        return jnp.dot(
            attended[final, rows, heads], late_w[final, heads, at], preferred_element_type=f32
        )

    for j in range(tiles // 2):
        at = slice(j * 2 * WIDE, (j + 1) * 2 * WIDE)
        total[:, at] = total[:, at] + fold_owner(every, at, col)

    for first in range(0, pieces, GROUP):
        group = range(first, min(first + GROUP, pieces))
        rows = slice(first * PIECE, (group[-1] + 1) * PIECE)
        for d in range(2):
            for i in group:
                cross_copy(d, final, i, 1 - col, la_recv.at[d, i]).wait_recv()
        for j in range(tiles // 2):
            at = slice(j * 2 * WIDE, (j + 1) * 2 * WIDE)
            out[rows, at] = (total[rows, at] + fold_owner(rows, at, 1 - col)).astype(bf16)

    for which in range(2):
        @pl.when(z != which * last_place)
        def _():
            stat_copy(which, z).wait_send()
    for d in range(2):
        pos = place(d)

        @pl.when(pos < last_place)
        def _():
            sent(gain_sum.at[d], gs_send.at[d])
            sent(summed.at[d], rs_send.at[d])

        @pl.when(pos > 0)
        def _():
            sent(wide_w.at[0, 0, pl.ds(0, pairs * tokens_n - DIRECT * PIECE)], at_send.at[d])

        @pl.when(pos == last_place)
        def _():
            sent(wide_w.at[0, 0, pl.ds(0, last_place * DIRECT * PIECE)], di_send)

    sent(summed.at[0, pl.ds(0, 2 * pairs)], la_send)
    for sem in (lx_send, ly_send, lc_send, ld_send):
        sent(late_w.at[0, pl.ds(0, 2 * pairs * quarter)], sem)


def fused_shards(rows_n, dp_n, tokens, norm_gain, qkv_weight, out_weight):
    tokens_n, block = tokens.shape
    pairs = qkv_weight.shape[2] // (2 * WIDE)
    chunks = 3 * pairs
    pieces = tokens_n // PIECE
    any_space = pl.BlockSpec(memory_space=pl.ANY)
    vmem = pl.BlockSpec(memory_space=pltpu.VMEM)
    hbm = pl.BlockSpec(memory_space=pltpu.HBM)
    dma = pltpu.SemaphoreType.DMA
    bf16, f32 = jnp.bfloat16, jnp.float32
    return pl.pallas_call(
        functools.partial(sublayer_kernel, rows_n, dp_n),
        out_shape=pltpu.VMEM((tokens_n, block), bf16),
        in_specs=[any_space, hbm, any_space, any_space],
        out_specs=vmem,
        scratch_shapes=[
            pltpu.VMEM((tokens_n, block), bf16),
            pltpu.VMEM((2, chunks, block, WIDE), bf16),
            pltpu.VMEM((block // 128, 128), f32),
            pltpu.VMEM((1, block), f32),
            pltpu.VMEM((2, tokens_n, 128), f32),
            pltpu.VMEM((rows_n, 2, 1, tokens_n), f32),
            pltpu.VMEM((rows_n + 1, tokens_n, 128), f32),
            pltpu.VMEM((tokens_n + EXTRA, block), bf16),
            pltpu.VMEM((2, 2, tokens_n, WIDE), f32),
            pltpu.VMEM((2, chunks, 1, WIDE), f32),
            pltpu.VMEM((chunks, rows_n, 1, WIDE), f32),
            pltpu.VMEM((2, chunks, tokens_n, WIDE), bf16),
            pltpu.VMEM((2, chunks, tokens_n, WIDE), bf16),
            pltpu.VMEM((pairs, tokens_n, 4 * WIDE), bf16),
            pltpu.VMEM((pairs, 4 * WIDE, block), bf16),
            pltpu.VMEM((tokens_n, block), f32),
            dma((pieces,)), dma, dma((2, chunks)), dma((pairs,)),
            dma((2,)), dma((rows_n,)), dma((2,)), dma((chunks,)),
            dma((2,)), dma((2, min(chunks * pieces, 2 * (LEAD + SKEW * (rows_n - 1) + pieces)))),
            dma((2,)), dma((2, pairs, pieces)), dma((2, pieces, 2)), dma, dma((pairs - 1,)),
            dma, dma((2, pieces)), dma, dma((pairs,)), dma, dma((pairs,)),
            dma, dma((pairs,)), dma, dma((pairs,)),
        ],
        compiler_params=pltpu.CompilerParams(
            collective_id=0, has_side_effects=True, vmem_limit_bytes=65800000
        ),
    )(
        tokens, norm_gain.reshape(block // 128, 128), jnp.transpose(qkv_weight, (1, 0, 2)),
        out_weight,
    )


def solution(mesh):
    in_specs = (P("dp", "row"), P("row"), P("row", None, "col"), P("col", "row"))
    out_specs = P("dp", "row")
    rows_n, cols_n, dp_n = mesh.shape["row"], mesh.shape["col"], mesh.shape["dp"]

    def body(tokens, norm_gain, qkv_weight, out_weight):
        tokens_n, block = tokens.shape
        fits = (
            cols_n == 2 and dp_n == 4 and rows_n >= 2 and qkv_weight.shape[2] % (2 * WIDE) == 0
            and qkv_weight.shape[2] >= 4 * WIDE
            and block % (2 * WIDE) == 0 and tokens_n % PIECE == 0
            and (qkv_weight.shape[2] // (2 * WIDE)) * tokens_n <= block
            and (rows_n - 1) * DIRECT * PIECE <= block and tokens_n > DIRECT * PIECE
        )
        if fits:
            return fused_shards(rows_n, dp_n, tokens, norm_gain, qkv_weight, out_weight)
        return shards(tokens, norm_gain, qkv_weight, out_weight)

    return jax.shard_map(body, mesh=mesh, in_specs=in_specs, out_specs=out_specs, check_vma=False)
```

```python
import functools
import math

import jax
import jax.numpy as jnp
from jax import lax
from jax.experimental import pallas as pl
from jax.experimental.pallas import tpu as pltpu
from jax.sharding import PartitionSpec as P

K = 128


EPSILON = 1e-05


def attend(queries, key_rows, value_rows):
    query_total = queries.shape[0]
    head_count = queries.shape[1] // K
    scaling = 1.0 / math.sqrt(K)
    split_keys = key_rows.reshape(key_rows.shape[0], head_count, K)
    split_values = value_rows.reshape(value_rows.shape[0], head_count, K)
    split_queries = queries.reshape(query_total, head_count, K)
    scores = (
        jnp.einsum("qhd,khd->hqk", split_queries, split_keys, preferred_element_type=jnp.float32)
        * scaling
    )
    largest = jnp.max(scores, axis=2, keepdims=True)
    exponent = jnp.exp(scores - largest)
    softmax_weights = (exponent / jnp.sum(exponent, axis=2, keepdims=True)).astype(jnp.bfloat16)
    mixed = jnp.einsum(
        "hqk,khd->qhd", softmax_weights, split_values, preferred_element_type=jnp.float32
    )
    result = mixed.astype(jnp.bfloat16)
    return result.reshape(query_total, head_count * K)


def shards(tokens, norm_gain, qkv_weight, out_weight):
    row_count, block_width = tokens.shape
    full_width = block_width * lax.axis_size("row")
    values = tokens.astype(jnp.float32)
    totals, squares = lax.psum(
        (jnp.sum(values, axis=1, keepdims=True), jnp.sum(values * values, axis=1, keepdims=True)),
        "row",
    )
    average = totals / full_width
    variance = squares / full_width - average * average
    centered = values - average
    normed = (centered * lax.rsqrt(variance + EPSILON) * norm_gain).astype(jnp.bfloat16)
    head_columns = qkv_weight.shape[2]
    partial_value = jnp.dot(
        normed,
        qkv_weight.reshape(block_width, 3 * head_columns),
        preferred_element_type=jnp.float32,
    )
    summed = lax.psum(partial_value.astype(jnp.bfloat16), "row").reshape(row_count, 3, head_columns)
    attended = attend(summed[:, 0], summed[:, 1], summed[:, 2])
    partial_out = jnp.dot(attended, out_weight, preferred_element_type=jnp.float32)
    return lax.psum(partial_out.astype(jnp.bfloat16), "col")


MESH = pl.DeviceIdType.MESH
WIDE = 2 * K
ROWS = 32
EXTRA = 16
PIECE = 96
GROUP = 2
DIRECT = 1
EARLY = 3
SKEW = 3
LEAD = 1
HAND = 20
HAND_ON = 34


def stream_blocks(pairs, pieces, lag):
    place, unit, blocks, asked = 0, 0, [], {}
    early = min(EARLY, pieces)
    while unit < 3 * pairs * pieces:
        following = len(blocks)
        if early and following < pairs - 2 and place >= asked.get(following, place + 1) + lag:
            blocks.append((following, 0, early, place))
            place += early
            continue
        if unit % (3 * pieces) == 2 * pieces:
            asked[unit // (3 * pieces)] = place
        unit += 1
        place += 1
    gone = len(blocks)
    for pair in range(pairs):
        first = early if pair < gone else 0
        if first < pieces:
            place = max(place, asked[pair] + first + lag)
            blocks.append((pair, first, pieces - first, place))
            place += pieces - first
    return blocks


def sublayer_kernel(
    rows_n, dp_n, tok_hbm, gain_hbm, w_hbm, wo_hbm, out,
    tok, wide_w, gain_ref, gain_row, stat_col, stats, spread_col, normed, part, gain_sum, gain_all,
    arrived, summed, attended, late_w, total,
    tok_sem, gain_sem, w_sem, late_sem, st_send, st_recv, gs_send, gs_recv, rs_send, rs_recv,
    at_send, at_recv, ah_recv, di_send, lp_recv, la_send, la_recv, lx_send, lx_recv, ly_send, ly_recv, lc_send, lc_recv,
    ld_send, ld_recv,
):
    z = lax.axis_index("row")
    col = lax.axis_index("col")
    dp = lax.axis_index("dp")
    tokens_n, block = tok.shape
    half = w_hbm.shape[2] // 2
    pairs = half // WIDE
    chunks = 3 * pairs
    pieces = tokens_n // PIECE
    units = chunks * pieces
    tiles = block // WIDE
    quarter = WIDE // dp_n
    partner = {"col": 1 - col}
    sibling_at = dp + 1 - 2 * (dp % 2)
    across_at = (dp + 2) % dp_n
    sibling, across = {"dp": sibling_at}, {"dp": across_at}
    scaling = 1.0 / math.sqrt(K)
    last_place = rows_n - 1
    f32, bf16 = jnp.float32, jnp.bfloat16

    def weight_copy(d, c):
        pair, kind = c // 3, (c + 1) % 3
        first = pl.multiple_of(d * half + pair * WIDE, WIDE)
        return pltpu.make_async_copy(
            w_hbm.at[kind, :, pl.ds(first, WIDE)], wide_w.at[d, c], w_sem.at[d, c]
        )

    gain_load = pltpu.make_async_copy(gain_hbm, gain_ref, gain_sem)
    gain_load.start()

    def tok_copy(i):
        rows = pl.ds(pl.multiple_of(i * PIECE, PIECE), PIECE)
        return pltpu.make_async_copy(tok_hbm.at[rows], tok.at[rows], tok_sem.at[i])

    @pl.loop(0, pieces)
    def _(i):
        tok_copy(i).start()

    early_side = jnp.where(2 * z < rows_n - 1, 1, 0)
    for c in range(2):
        weight_copy(early_side, c).start()
    for c in range(2):
        weight_copy(1 - early_side, c).start()

    @pl.loop(2, chunks)
    def _(c):
        weight_copy(0, c).start()
        weight_copy(1, c).start()

    def head_columns(owner, d):
        return pl.ds(pl.multiple_of((owner * 2 + d) * WIDE, WIDE), WIDE)

    def own_copy(d, p):
        rows = pl.ds(d * half + p * WIDE, WIDE)
        return pltpu.make_async_copy(
            wo_hbm.at[rows], late_w.at[p, head_columns(col, d)], late_sem.at[p]
        )

    def quarter_at(owner, d, which):
        first = (owner * 2 + d) * WIDE + which * quarter
        return pl.ds(pl.multiple_of(first, quarter), quarter)

    def share_copy(d, p, owner):
        first = pl.multiple_of(d * half + p * WIDE + dp * quarter, quarter)
        return pltpu.make_async_remote_copy(
            src_ref=wo_hbm.at[pl.ds(first, quarter)],
            dst_ref=late_w.at[p, quarter_at(owner, d, dp)],
            send_sem=lx_send, recv_sem=lx_recv.at[p], device_id=partner,
            device_id_type=MESH,
        )

    def pass_copy(d, p, which, sends, recvs, device):
        piece = late_w.at[p, quarter_at(1 - col, d, which)]
        return pltpu.make_async_remote_copy(
            src_ref=piece, dst_ref=piece, send_sem=sends, recv_sem=recvs.at[p],
            device_id=device, device_id_type=MESH,
        )

    def across_copy(d, p, which):
        return pass_copy(d, p, which, ly_send, ly_recv, across)

    def near_copy(d, p, which):
        return pass_copy(d, p, which, lc_send, lc_recv, sibling)

    def far_copy(d, p, which):
        return pass_copy(d, p, which, ld_send, ld_recv, sibling)

    def whole(source, sem):
        return pltpu.make_async_remote_copy(
            src_ref=source, dst_ref=source, send_sem=sem, recv_sem=sem,
            device_id=partner, device_id_type=MESH,
        )

    def sent(source, sem):
        whole(source, sem).wait_send()

    def landed(target, sem):
        whole(target, sem).wait_recv()

    @pl.loop(0, pairs)
    def _(p):
        own_copy(0, p).start()
        own_copy(1, p).start()

    barrier = pltpu.get_barrier_semaphore()
    for o in range(1, rows_n):
        pl.semaphore_signal(
            barrier, inc=1, device_id={"row": lax.rem(z + o, rows_n)}, device_id_type=MESH
        )
    for device in (partner, sibling, across):
        pl.semaphore_signal(barrier, inc=1, device_id=device, device_id_type=MESH)

    gain_load.wait()
    for j in range(block // 128):
        gain_row[0:1, j * 128:(j + 1) * 128] = gain_ref[j:j + 1, :]
    gain = gain_row[...]
    high = gain.astype(bf16).astype(f32)
    row = lax.broadcasted_iota(jnp.int32, (EXTRA, block), 0)
    normed[pl.ds(tokens_n, EXTRA), :] = jnp.where(
        row == 0, high, jnp.where(row == 1, gain - high, 0.0)
    ).astype(bf16)
    def place(d):
        return jnp.where(d == 1, z, last_place - z)

    def end_of(d):
        return jnp.where(d == 1, last_place, 0)

    def onward(d):
        return {"row": jnp.clip(jnp.where(d == 1, z + 1, z - 1), 0, last_place)}

    def back(d):
        return {"row": jnp.clip(jnp.where(d == 1, z - 1, z + 1), 0, last_place)}

    def stat_copy(which, source):
        return pltpu.make_async_remote_copy(
            src_ref=stats.at[source], dst_ref=stats.at[source], send_sem=st_send.at[which],
            recv_sem=st_recv.at[source], device_id={"row": which * last_place},
            device_id_type=MESH,
        )

    def gain_copy(d, c, source):
        return pltpu.make_async_remote_copy(
            src_ref=gain_sum.at[d, c], dst_ref=gain_all.at[c, source], send_sem=gs_send.at[d],
            recv_sem=gs_recv.at[c], device_id={"row": end_of(d)}, device_id_type=MESH,
        )

    def sum_copy(d, c, i):
        at = pl.ds(pl.multiple_of(i * PIECE, PIECE), PIECE)
        return pltpu.make_async_remote_copy(
            src_ref=summed.at[d, c, at], dst_ref=arrived.at[d, c, at],
            send_sem=rs_send.at[d], recv_sem=rs_recv.at[d, (c * pieces + i) % rs_recv.shape[1]],
            device_id=onward(d), device_id_type=MESH,
        )

    def attended_part(owner, d, p, i):
        rows = pl.ds(pl.multiple_of(i * PIECE, PIECE), PIECE)
        return attended.at[p, rows, head_columns(owner, d)]

    def attended_copy(d, p, i):
        piece = attended_part(col, d, p, i)
        return pltpu.make_async_remote_copy(
            src_ref=piece, dst_ref=piece, send_sem=at_send.at[d],
            recv_sem=at_recv.at[d, p, i], device_id=back(d), device_id_type=MESH,
        )

    def half_part(owner, d, i, h):
        first = pl.multiple_of(i * PIECE + h * (PIECE // 2), PIECE // 2)
        return attended.at[pairs - 1, pl.ds(first, PIECE // 2), head_columns(owner, d)]

    def half_copy(d, i, h):
        piece = half_part(col, d, i, h)
        return pltpu.make_async_remote_copy(
            src_ref=piece, dst_ref=piece, send_sem=at_send.at[d],
            recv_sem=ah_recv.at[d, i, h], device_id=back(d), device_id_type=MESH,
        )

    def half_cross(d, i, h):
        piece = half_part(col, d, i, h)
        return pltpu.make_async_remote_copy(
            src_ref=piece, dst_ref=piece, send_sem=la_send,
            recv_sem=la_recv.at[d, i], device_id=partner, device_id_type=MESH,
        )

    def direct_copy(d, p, i, o):
        piece = attended_part(col, d, p, i)
        return pltpu.make_async_remote_copy(
            src_ref=piece, dst_ref=piece, send_sem=di_send,
            recv_sem=at_recv.at[d, p, i],
            device_id={"row": jnp.clip(jnp.where(d == 1, z - o, z + o), 0, last_place)},
            device_id_type=MESH,
        )

    def cross_copy(d, p, i, owner, recv_sem):
        piece = attended_part(owner, d, p, i)
        return pltpu.make_async_remote_copy(
            src_ref=piece, dst_ref=piece, send_sem=la_send,
            recv_sem=recv_sem, device_id=partner, device_id_type=MESH,
        )

    def cross_over(d, p, i):
        @pl.when(p < pairs - 1)
        def _():
            cross_copy(d, p, i, col, lp_recv.at[jnp.minimum(p, pairs - 2)]).start()

        @pl.when(p == pairs - 1)
        def _():
            cross_copy(d, p, i, col, la_recv.at[d, i]).start()

    def attend_piece(d, p, i):
        rows = pl.ds(pl.multiple_of(i * PIECE, PIECE), PIECE)
        first = (col * 2 + d) * WIDE
        for h in range(2):
            at = slice(h * K, (h + 1) * K)
            k = summed[d, 3 * p, :, at]
            v = summed[d, 3 * p + 1, :, at]
            q = summed[d, 3 * p + 2, rows, at]
            scores = lax.dot_general(
                q, k, (((1,), (1,)), ((), ())), preferred_element_type=f32
            )
            exponent = jnp.exp2(
                (scores - jnp.max(scores, axis=1, keepdims=True)) * (scaling * math.log2(math.e))
            )
            mixed = jnp.dot(exponent.astype(bf16), v, preferred_element_type=f32)
            attended[p, rows, pl.ds(pl.multiple_of(first + h * K, K), K)] = (
                mixed / jnp.sum(exponent, axis=1, keepdims=True)
            ).astype(bf16)

    def spread_statistics():
        for o in range(1, rows_n):
            stat_copy(0, lax.rem(z + o, rows_n)).wait_recv()
        mean = sum(stats[i, 0] for i in range(rows_n)) * (1.0 / rows_n)
        spread = sum(
            stats[i, 1] * (1.0 / block) + (stats[i, 0] - mean) * (stats[i, 0] - mean)
            for i in range(rows_n)
        ) * (1.0 / rows_n)
        scale = lax.rsqrt(spread + EPSILON)
        for i in range(rows_n):
            shift = (stats[i, 0] - mean) * scale
            spread_col[i] = jnp.broadcast_to(shift, (128, tokens_n)).T
        spread_col[rows_n] = jnp.broadcast_to(scale, (128, tokens_n)).T

    def weights_ready(p):
        rows = late_w.at[p, pl.ds(0, 2 * WIDE)]
        pltpu.make_async_copy(rows, rows, late_sem.at[p]).wait()
        for recvs in (lc_recv, ld_recv):
            landed(late_w.at[p, pl.ds(0, 2 * quarter)], recvs.at[p])

    def pair_ready(p):
        weights_ready(p)
        landed(summed.at[0, pl.ds(0, 2)], lp_recv.at[p])

    def fold(p, rows, at):
        return jnp.dot(attended[p, rows, :], late_w[p, :, at], preferred_element_type=f32)

    nearer = jnp.where(z < last_place - z, 1, 0)
    starts = (z == 0) | (z == last_place)

    def centre(i):
        tok_copy(i).wait()

        @pl.loop(0, PIECE // ROWS)
        def _(j):
            at = pl.ds(pl.multiple_of(i * PIECE + j * ROWS, ROWS), ROWS)
            x = tok[at, :].astype(f32)
            mean = jnp.sum(x, axis=1, keepdims=True) * (1.0 / block)
            away = x - mean
            square = jnp.sum(away * away, axis=1, keepdims=True)
            normed[at, :] = (away * gain_row[...]).astype(bf16)
            stat_col[0, at, :] = jnp.broadcast_to(mean, (ROWS, 128))
            stat_col[1, at, :] = jnp.broadcast_to(square, (ROWS, 128))

    def first_piece(i):
        rows = pl.ds(pl.multiple_of(i * PIECE, PIECE), PIECE)
        summed[nearer, 0, rows] = jnp.dot(
            normed[rows, :], wide_w[nearer, 0], preferred_element_type=f32
        ).astype(bf16)

    centre(0)

    @pl.when(starts)
    def _():
        weight_copy(nearer, 0).wait()
        first_piece(0)

    pl.semaphore_wait(barrier, rows_n + 2)

    @pl.when(starts)
    def _():
        sum_copy(nearer, 0, 0).start()


    @pl.loop(1, pieces)
    def _(i):
        centre(i)

        @pl.when(starts)
        def _():
            first_piece(i)
            sum_copy(nearer, 0, i).start()

    @pl.when(starts)
    def _():
        value = jnp.dot(
            normed[pl.ds(tokens_n, EXTRA), :], wide_w[nearer, 0], preferred_element_type=f32
        )
        gain_sum[nearer, 0] = value[0:1] + value[1:2]
        gain_copy(nearer, 0, z).start()

    def offset(pos):
        return jnp.where(pos > 0, LEAD + SKEW * pos, -pieces)

    end_offset = LEAD + SKEW * last_place
    blocks = stream_blocks(pairs, pieces, end_offset + pieces + 1)
    slots = blocks[-1][3] + pieces + end_offset
    every = pl.ds(0, tokens_n)

    def fold_pair(p):
        pair_ready(p)
        for j in range(tiles // 2):
            at = slice(j * 2 * WIDE, (j + 1) * 2 * WIDE)
            value = fold(p, every, at)
            total[:, at] = value if p == 0 else total[:, at] + value

    stat_slot = jnp.where(starts, 0, LEAD + SKEW + 1)

    def multiply(d, c, pos):
        weight_copy(d, c).wait()
        value = jnp.dot(normed[...], wide_w[d, c], preferred_element_type=f32)
        part[d, c % 2] = value[0:tokens_n]
        gain_value = value[tokens_n:tokens_n + 1] + value[tokens_n + 1:tokens_n + 2]

        @pl.when(pos < last_place)
        def _():
            gain_sum[d, c] = gain_value
            gain_copy(d, c, z).start()

        @pl.when(pos == last_place)
        def _():
            gain_all[c, z] = gain_value

    @pl.when(starts)
    def _():
        multiply(nearer, 1, 0)

    @pl.loop(0, slots)
    def _(t):
        @pl.when(t == stat_slot + 4)
        def _():
            @pl.loop(0, pairs)
            def _(p):
                share_copy(0, p, col).start()
                share_copy(1, p, col).start()

        @pl.when(t == stat_slot)
        def _():
            stats[z, 0] = stat_col[0].T[0:1]
            stats[z, 1] = stat_col[1].T[0:1]
            for which in range(2):
                @pl.when(z != which * last_place)
                def _():
                    stat_copy(which, z).start()

        @pl.when((t == end_offset - 1) & starts)
        def _():
            spread_statistics()

        ahead = []
        for k in range(2):
            d = nearer if k == 0 else 1 - nearer
            pos = place(d)
            n = t - offset(pos)
            u = n
            returns = False
            back_pair, back_piece = 0, 0
            for p, piece, count, begin in blocks:
                inside = (n >= begin) & (n < begin + count)
                returns = returns | inside
                back_pair = jnp.where(inside, p, back_pair)
                back_piece = jnp.where(inside, n - begin + piece, back_piece)
                u = jnp.where(n >= begin + count, u - count, u)
            c, i = u // pieces, u % pieces

            @pl.when((u >= 0) & (u < units) & jnp.logical_not(returns))
            def _():
                rows = pl.ds(pl.multiple_of(i * PIECE, PIECE), PIECE)

                side = c % 2

                @pl.when((i == 0) & (pos == last_place))
                def _():
                    landed(gain_all.at[c, pl.ds(0, last_place)], gs_recv.at[c])

                @pl.when(pos == 0)
                def _():
                    summed[d, c, rows] = part[d, side, rows].astype(bf16)

                @pl.when(pos > 0)
                def _():
                    sum_copy(d, c, i).wait_recv()

                @pl.when((pos > 0) & (pos < last_place))
                def _():
                    summed[d, c, rows] = (part[d, side, rows] + arrived[d, c, rows].astype(f32)).astype(bf16)

                @pl.when(pos < last_place)
                def _():
                    sum_copy(d, c, i).start()

                @pl.when(pos == last_place)
                def _():
                    scale = spread_col[rows_n, rows]
                    for h in range(2):
                        lanes = slice(h * 128, (h + 1) * 128)
                        whole = part[d, side, rows, lanes] + arrived[d, c, rows, lanes].astype(f32)
                        whole = whole * scale
                        for source in range(rows_n):
                            whole = whole + spread_col[source, rows] * gain_all[c, source, :, lanes]
                        summed[d, c, rows, lanes] = whole.astype(bf16)

                @pl.when((pos == last_place) & (c % 3 == 2))
                def _():
                    attend_piece(d, c // 3, i)
                    cross_over(d, c // 3, i)

            ahead.append(
                (d, pos, u + 1, (u >= -1) & (u < units - 1) & jnp.logical_not(returns))
            )

            @pl.when(returns)
            def _():
                p, other = back_pair, 1 - d
                turned = (p == pairs - 1) & (pos == last_place)
                s = jnp.where(turned, (back_piece + pieces - DIRECT) % pieces, back_piece)
                direct = (p == pairs - 1) & (s >= pieces - DIRECT)

                halved = (p == pairs - 1) & jnp.logical_not(direct)

                @pl.when(halved)
                def _():
                    for h in range(2):
                        @pl.when(pos > 0)
                        def _():
                            half_copy(other, s, h).wait_recv()

                        @pl.when(pos < last_place)
                        def _():
                            half_copy(other, s, h).start()

                        @pl.when(pos > 0)
                        def _():
                            half_cross(other, s, h).start()

                @pl.when(jnp.logical_not(halved) & (pos > 0))
                def _():
                    attended_copy(other, p, s).wait_recv()

                @pl.when((pos < last_place) & jnp.logical_not(halved | direct))
                def _():
                    attended_copy(other, p, s).start()

                @pl.when((pos == 0) & direct)
                def _():
                    for o in range(last_place, 0, -1):
                        direct_copy(other, p, s, o).start()

                @pl.when(jnp.logical_not(halved) & (pos > 0))
                def _():
                    cross_over(other, p, s)

        for d, pos, u, due in ahead:
            @pl.when(due & (u % pieces == 0))
            def _():
                multiply(d, u // pieces, pos)

        @pl.when((t >= HAND) & (t < HAND + 2 * pieces * pairs) & ((t - HAND) % (2 * pieces) == 0))
        def _():
            p = (t - HAND) // (2 * pieces)
            landed(late_w.at[p, pl.ds(0, 2 * quarter)], lx_recv.at[p])
            for d in range(2):
                across_copy(d, p, dp).start()
                near_copy(d, p, dp).start()

        @pl.when(
            (t >= HAND_ON) & (t < HAND_ON + 2 * pieces * pairs)
            & ((t - HAND_ON) % (2 * pieces) == 0)
        )
        def _():
            p = (t - HAND_ON) // (2 * pieces)
            landed(late_w.at[p, pl.ds(0, 2 * quarter)], ly_recv.at[p])
            for d in range(2):
                far_copy(d, p, across_at).start()

        @pl.when(t == blocks[-2][3] + blocks[-2][2] + end_offset)
        def _():
            for p in range(pairs - 2):
                fold_pair(p)

    final = pairs - 1
    fold_pair(final - 1)
    weights_ready(final)

    def fold_owner(rows, at, owner):
        heads = pl.ds(pl.multiple_of(owner * 2 * WIDE, 2 * WIDE), 2 * WIDE)
        return jnp.dot(
            attended[final, rows, heads], late_w[final, heads, at], preferred_element_type=f32
        )

    for j in range(tiles // 2):
        at = slice(j * 2 * WIDE, (j + 1) * 2 * WIDE)
        total[:, at] = total[:, at] + fold_owner(every, at, col)

    for first in range(0, pieces, GROUP):
        group = range(first, min(first + GROUP, pieces))
        rows = slice(first * PIECE, (group[-1] + 1) * PIECE)
        for d in range(2):
            for i in group:
                cross_copy(d, final, i, 1 - col, la_recv.at[d, i]).wait_recv()
        for j in range(tiles // 2):
            at = slice(j * 2 * WIDE, (j + 1) * 2 * WIDE)
            out[rows, at] = (total[rows, at] + fold_owner(rows, at, 1 - col)).astype(bf16)

    for which in range(2):
        @pl.when(z != which * last_place)
        def _():
            stat_copy(which, z).wait_send()
    for d in range(2):
        pos = place(d)

        @pl.when(pos < last_place)
        def _():
            sent(gain_sum.at[d], gs_send.at[d])
            sent(summed.at[d], rs_send.at[d])

        @pl.when(pos > 0)
        def _():
            sent(wide_w.at[0, 0, pl.ds(0, pairs * tokens_n - DIRECT * PIECE)], at_send.at[d])

        @pl.when(pos == last_place)
        def _():
            sent(wide_w.at[0, 0, pl.ds(0, last_place * DIRECT * PIECE)], di_send)

    sent(summed.at[0, pl.ds(0, 2 * pairs)], la_send)
    for sem in (lx_send, ly_send, lc_send, ld_send):
        sent(late_w.at[0, pl.ds(0, 2 * pairs * quarter)], sem)


def fused_shards(rows_n, dp_n, tokens, norm_gain, qkv_weight, out_weight):
    tokens_n, block = tokens.shape
    pairs = qkv_weight.shape[2] // (2 * WIDE)
    chunks = 3 * pairs
    pieces = tokens_n // PIECE
    any_space = pl.BlockSpec(memory_space=pl.ANY)
    vmem = pl.BlockSpec(memory_space=pltpu.VMEM)
    hbm = pl.BlockSpec(memory_space=pltpu.HBM)
    dma = pltpu.SemaphoreType.DMA
    bf16, f32 = jnp.bfloat16, jnp.float32
    return pl.pallas_call(
        functools.partial(sublayer_kernel, rows_n, dp_n),
        out_shape=pltpu.VMEM((tokens_n, block), bf16),
        in_specs=[any_space, hbm, any_space, any_space],
        out_specs=vmem,
        scratch_shapes=[
            pltpu.VMEM((tokens_n, block), bf16),
            pltpu.VMEM((2, chunks, block, WIDE), bf16),
            pltpu.VMEM((block // 128, 128), f32),
            pltpu.VMEM((1, block), f32),
            pltpu.VMEM((2, tokens_n, 128), f32),
            pltpu.VMEM((rows_n, 2, 1, tokens_n), f32),
            pltpu.VMEM((rows_n + 1, tokens_n, 128), f32),
            pltpu.VMEM((tokens_n + EXTRA, block), bf16),
            pltpu.VMEM((2, 2, tokens_n, WIDE), f32),
            pltpu.VMEM((2, chunks, 1, WIDE), f32),
            pltpu.VMEM((chunks, rows_n, 1, WIDE), f32),
            pltpu.VMEM((2, chunks, tokens_n, WIDE), bf16),
            pltpu.VMEM((2, chunks, tokens_n, WIDE), bf16),
            pltpu.VMEM((pairs, tokens_n, 4 * WIDE), bf16),
            pltpu.VMEM((pairs, 4 * WIDE, block), bf16),
            pltpu.VMEM((tokens_n, block), f32),
            dma((pieces,)), dma, dma((2, chunks)), dma((pairs,)),
            dma((2,)), dma((rows_n,)), dma((2,)), dma((chunks,)),
            dma((2,)), dma((2, min(chunks * pieces, 2 * (LEAD + SKEW * (rows_n - 1) + pieces)))),
            dma((2,)), dma((2, pairs, pieces)), dma((2, pieces, 2)), dma, dma((pairs - 1,)),
            dma, dma((2, pieces)), dma, dma((pairs,)), dma, dma((pairs,)),
            dma, dma((pairs,)), dma, dma((pairs,)),
        ],
        compiler_params=pltpu.CompilerParams(
            collective_id=0, has_side_effects=True, vmem_limit_bytes=65800000
        ),
    )(
        tokens, norm_gain.reshape(block // 128, 128), jnp.transpose(qkv_weight, (1, 0, 2)),
        out_weight,
    )


def solution(mesh):
    in_specs = (P("dp", "row"), P("row"), P("row", None, "col"), P("col", "row"))
    out_specs = P("dp", "row")
    rows_n, cols_n, dp_n = mesh.shape["row"], mesh.shape["col"], mesh.shape["dp"]

    def body(tokens, norm_gain, qkv_weight, out_weight):
        tokens_n, block = tokens.shape
        fits = (
            cols_n == 2 and dp_n == 4 and rows_n >= 2 and qkv_weight.shape[2] % (2 * WIDE) == 0
            and qkv_weight.shape[2] >= 4 * WIDE
            and block % (2 * WIDE) == 0 and tokens_n % PIECE == 0
            and (qkv_weight.shape[2] // (2 * WIDE)) * tokens_n <= block
            and (rows_n - 1) * DIRECT * PIECE <= block and tokens_n > DIRECT * PIECE
        )
        if fits:
            return fused_shards(rows_n, dp_n, tokens, norm_gain, qkv_weight, out_weight)
        return shards(tokens, norm_gain, qkv_weight, out_weight)

    return jax.shard_map(body, mesh=mesh, in_specs=in_specs, out_specs=out_specs, check_vma=False)
```
